32 devices in a mesh: seq: 8 (over z, y), tensor: 4 (over x, core).
Axes of the slice: x: 2, y: 2, z: 4, core: 2. Of those that a mesh axis runs over, the one named last changes fastest.
Arguments:
- fixed_point: bfloat16 [1024, 4096], P(('seq', 'tensor')), may hold values from -6 to 6
- incoming: bfloat16 [1024, 4096], P(('seq', 'tensor')), may hold values from -6 to 6
- norm_gain: float32 [4096], replicated, may hold values from 0.1 to 1.9
- query_weight: bfloat16 [4096, 4096], P(None, 'tensor'), may hold values from -0.21875 to 0.21875, as said below
- key_weight: bfloat16 [4096, 4096], P(None, 'tensor'), may hold values from -0.265625 to 0.265625, as said below
- value_weight: bfloat16 [4096, 4096], P(None, 'tensor'), may hold values from -0.09375 to 0.09375
- out_weight: bfloat16 [4096, 4096], P('tensor'), may hold values from -0.09375 to 0.09375
- layout: int32 [16, 16], replicated, may hold values 0 or 1
Outputs:
- adjoint: float32 [1024, 4096], P(('seq', 'tensor'))
- gain_grad: float32 [4096], replicated
The draws below stay inside these ranges and needn't reach their ends.
Inputs may be any that keep to these rules, and one draw needn't show every extreme that they name: `query_weight`: entries of the columns of each head are independent; their spread may differ between heads. `key_weight`: entries are independent within a draw; columns of some heads may follow the same head's columns of query_weight. `layout`: A key block strictly before a query block is attended where the entry at row query block, column key block is 1; a block always attends itself causally; entries on or above the diagonal are not read.
All inputs are finite; a program needn't handle non-finite values.
Results may differ from the reference program's by a relative error of at most 0.03.
Values may be sent and summed in bfloat16 or wider, within the bound.
A program may use at most 128 MiB of HBM per device.

```python
import jax
import jax.numpy as jnp
from jax import lax

D = 4096
HEADS = 32
HEAD_DIM = 128
BLK = 64
ITERS = 2
HEADS_DEV = 8
LENGTH = 1024
NBLK = 16


def projection_pair(key):
    first = jax.random.truncated_normal(jax.random.fold_in(key, 11), -4.0, 4.0, (D, D), jnp.float32)
    second = jax.random.truncated_normal(jax.random.fold_in(key, 23), -4.0, 4.0, (D, D), jnp.float32)
    plain = (2.0 / D) ** 0.5
    query = first * plain
    keyed = second * plain
    return (query, keyed)


def draw_query_weight(key, part):
    return projection_pair(key)[0].astype(jnp.bfloat16)


def draw_key_weight(key, part):
    return projection_pair(key)[1].astype(jnp.bfloat16)


def set_ends(values, stream_key, least, top_value):
    shape = values.shape
    place = [jax.random.randint(jax.random.fold_in(stream_key, axis), (), 0, shape[axis]) for axis in range(len(shape))]
    values = values.at[tuple(place)].set(least)
    longest = shape.index(max(shape))
    place[longest] = (place[longest] + 1) % shape[longest]
    return values.at[tuple(place)].set(top_value)


def block_levels(own_key, shape, cuts, smallest, top_value):
    def one(dim, parts):
        heights = jax.random.uniform(jax.random.fold_in(jax.random.fold_in(own_key, 6), dim), (parts,), jnp.float32, smallest / len(cuts), top_value / len(cuts))
        return jnp.repeat(jnp.exp(heights), shape[dim] // parts).reshape((-1,) + (1,) * (len(shape) - dim - 1))

    loudness = one(*cuts[0])
    for cut in cuts[1:]:
        loudness = loudness * one(*cut)
    return loudness


def noise(stream_key, dims, scale, bound, cuts=(), kind=jnp.bfloat16):
    values = scale * jax.random.normal(stream_key, dims, jnp.float32)
    if cuts:
        values = values * block_levels(stream_key, dims, cuts, -0.22, 0.18)
    return jnp.clip(values, -bound, bound).astype(kind)


def setup_inputs(seed: int = 0) -> dict:
    splits = jax.random.split(jax.random.key(seed), 9)
    fixed_point = noise(splits[0], (LENGTH, D), 1.0, 6.0, ((0, 32),))
    incoming = noise(splits[1], (LENGTH, D), 1.0, 6.0, ((0, 32),))
    norm_gain = jnp.clip(1.0 + 0.18 * jax.random.normal(splits[2], (D,), jnp.float32), 0.1, 1.9)
    query_weight = draw_query_weight(jax.random.fold_in(splits[8], 71), 0)
    key_weight = draw_key_weight(jax.random.fold_in(splits[8], 71), 0)
    value_weight = noise(splits[5], (D, D), D ** -0.5, 0.09375, ((1, 4),))
    out_weight = noise(splits[6], (D, D), D ** -0.5, 0.09375, ((0, 4),))
    layout = set_ends((jax.random.randint(splits[7], (NBLK, NBLK), 0, 4) < 3).astype(jnp.int32), jax.random.fold_in(splits[7], 1), 0, 1)
    return dict(fixed_point=fixed_point, incoming=incoming, norm_gain=norm_gain, query_weight=query_weight, key_weight=key_weight, value_weight=value_weight, out_weight=out_weight, layout=layout)


EPS = 1e-05
THETA = 10000.0
MASKED = -1e+30

def round_low(values):
    return lax.optimization_barrier(values.astype(jnp.bfloat16)).astype(jnp.float32)

def rope_tables(positions):
    freq = THETA ** (-jnp.arange(0, HEAD_DIM, 2, dtype=jnp.float32) / HEAD_DIM)
    angle = positions.astype(jnp.float32)[:, None] * freq[None, :]
    cosine = jnp.concatenate([jnp.cos(angle), jnp.cos(angle)], axis=1)[:, None, :]
    sine = jnp.concatenate([jnp.sin(angle), jnp.sin(angle)], axis=1)[:, None, :]
    return (cosine, sine)

def rotate(values, cosine, sine):
    half = HEAD_DIM // 2
    turned = jnp.concatenate([-values[..., half:], values[..., :half]], axis=-1)
    return values * cosine + turned * sine

def rotate_back(values, cosine, sine):
    half = HEAD_DIM // 2
    weighted = values * sine
    turned = jnp.concatenate([weighted[..., half:], -weighted[..., :half]], axis=-1)
    return values * cosine + turned

def expand_blocks(chosen):
    return jnp.repeat(jnp.repeat(chosen, BLK, axis=0), BLK, axis=1)

def pair_mask(query_pos, key_pos, chosen):
    query_block = (query_pos // BLK)[:, None]
    key_block = (key_pos // BLK)[None, :]
    earlier = (key_block < query_block) & chosen
    same = (key_block == query_block) & (key_pos[None, :] <= query_pos[:, None])
    return earlier | same

def reference(fixed_point, incoming, norm_gain, query_weight, key_weight, value_weight, out_weight, layout):
    groups = HEADS // HEADS_DEV
    width = HEADS_DEV * HEAD_DIM
    score_scale = HEAD_DIM ** (-0.5)
    point = fixed_point.astype(jnp.float32)
    inv_rms = lax.rsqrt(lax.optimization_barrier(jnp.mean(point * point, axis=1, keepdims=True)) + EPS)
    scaled = point * inv_rms
    normed = (norm_gain * scaled).astype(jnp.bfloat16)
    positions = jnp.arange(LENGTH, dtype=jnp.int32)
    cosine, sine = rope_tables(positions)

    def project(weight):
        return jnp.dot(normed, weight, preferred_element_type=jnp.float32).reshape(LENGTH, HEADS, HEAD_DIM)

    def split_heads(values):
        return values.reshape(LENGTH, groups, HEADS_DEV, HEAD_DIM).transpose(1, 0, 2, 3)
    queries = split_heads(rotate(project(query_weight), cosine, sine).astype(jnp.bfloat16))
    keys = split_heads(rotate(project(key_weight), cosine, sine).astype(jnp.bfloat16))
    values = split_heads(project(value_weight).astype(jnp.bfloat16))
    allowed = pair_mask(positions, positions, expand_blocks(layout > 0))[None]

    def probabilities(query_group, key_group):
        scores = jnp.einsum('qhd,khd->hqk', query_group.astype(jnp.float32), key_group.astype(jnp.float32)) * score_scale
        scores = jnp.where(allowed, scores, MASKED)
        return jnp.exp(scores - jax.nn.logsumexp(scores, axis=2, keepdims=True))

    def forward_group(operands):
        query_group, key_group, value_group = operands
        probs = probabilities(query_group, key_group)
        attended = jnp.einsum('hqk,khd->qhd', round_low(probs), value_group.astype(jnp.float32))
        return attended.astype(jnp.bfloat16)
    attended = lax.map(forward_group, (queries, keys, values))
    query_cols = query_weight.reshape(D, groups, width).transpose(1, 0, 2)
    key_cols = key_weight.reshape(D, groups, width).transpose(1, 0, 2)
    value_cols = value_weight.reshape(D, groups, width).transpose(1, 0, 2)
    out_rows = out_weight.reshape(groups, width, D)

    def backprop(cotangent):
        cotangent_low = cotangent.astype(jnp.bfloat16)

        def group_step(total, operands):
            query_group, key_group, value_group, attended_group, query_col, key_col, value_col, out_row = operands
            grad_out = jnp.dot(cotangent_low, out_row.T, preferred_element_type=jnp.float32).astype(jnp.bfloat16)
            grad_wide = grad_out.astype(jnp.float32).reshape(LENGTH, HEADS_DEV, HEAD_DIM)
            delta = lax.optimization_barrier(jnp.sum(grad_wide * attended_group.astype(jnp.float32), axis=2)).T
            probs = probabilities(query_group, key_group)
            grad_probs = jnp.einsum('qhd,khd->hqk', grad_wide, value_group.astype(jnp.float32))
            grad_scores = round_low(probs * (grad_probs - delta[:, :, None]))
            grad_query = jnp.einsum('hqk,khd->qhd', grad_scores, key_group.astype(jnp.float32)) * score_scale
            grad_key = jnp.einsum('hqk,qhd->khd', grad_scores, query_group.astype(jnp.float32)) * score_scale
            grad_value = jnp.einsum('hqk,qhd->khd', round_low(probs), grad_wide)
            query_low = rotate_back(grad_query, cosine, sine).astype(jnp.bfloat16).reshape(LENGTH, width)
            key_low = rotate_back(grad_key, cosine, sine).astype(jnp.bfloat16).reshape(LENGTH, width)
            value_low = grad_value.astype(jnp.bfloat16).reshape(LENGTH, width)
            partial_sum = jnp.dot(query_low, query_col.T, preferred_element_type=jnp.float32)
            partial_sum = partial_sum + jnp.dot(key_low, key_col.T, preferred_element_type=jnp.float32)
            partial_sum = partial_sum + jnp.dot(value_low, value_col.T, preferred_element_type=jnp.float32)
            return (total + round_low(partial_sum), None)
        operands = (queries, keys, values, attended, query_cols, key_cols, value_cols, out_rows)
        grad_normed, _ = lax.scan(group_step, jnp.zeros((LENGTH, D), jnp.float32), operands)
        return grad_normed
    cotangent = incoming.astype(jnp.float32)
    adjoint = cotangent
    gain_total = jnp.zeros((D,), jnp.float32)
    for term_index in range(ITERS):
        grad_normed = backprop(cotangent)
        gain_total = gain_total + lax.optimization_barrier(jnp.sum(grad_normed * scaled, axis=0))
        weighted = norm_gain * grad_normed
        inner = lax.optimization_barrier(jnp.sum(weighted * scaled, axis=1, keepdims=True))
        cotangent = inv_rms * (weighted - scaled * (inner / D))
        adjoint = adjoint + cotangent
    return (adjoint, gain_total * LENGTH ** (-0.5))
```

```python
import types

import jax
import jax.numpy as jnp
import numpy as np
from jax import lax
from jax.experimental import pallas as pl
from jax.experimental.pallas import tpu as pltpu
from jax.sharding import PartitionSpec as P

HEAD_DIM = 128
BLK = 64
ITERS = 2


EPS = 1e-05
THETA = 10000.0
MASKED = -1e30


def rope_tables(positions):
    freq = THETA ** (-jnp.arange(0, HEAD_DIM, 2, dtype=jnp.float32) / HEAD_DIM)
    angle = positions.astype(jnp.float32)[:, None] * freq[None, :]
    cosine = jnp.concatenate([jnp.cos(angle), jnp.cos(angle)], axis=1)[:, None, :]
    sine = jnp.concatenate([jnp.sin(angle), jnp.sin(angle)], axis=1)[:, None, :]
    return (cosine, sine)


def rotate(values, cosine, sine):
    half = HEAD_DIM // 2
    turned = jnp.concatenate([-values[..., half:], values[..., :half]], axis=-1)
    return values * cosine + turned * sine


def rotate_back(values, cosine, sine):
    half = HEAD_DIM // 2
    weighted = values * sine
    turned = jnp.concatenate([weighted[..., half:], -weighted[..., :half]], axis=-1)
    return values * cosine + turned


def expand_blocks(chosen):
    return jnp.repeat(jnp.repeat(chosen, BLK, axis=0), BLK, axis=1)


def pair_mask(query_pos, key_pos, chosen):
    query_block = (query_pos // BLK)[:, None]
    key_block = (key_pos // BLK)[None, :]
    earlier = (key_block < query_block) & chosen
    same = (key_block == query_block) & (key_pos[None, :] <= query_pos[:, None])
    return earlier | same


def ring_body(
    fixed_point, incoming, norm_gain, query_weight, key_weight, value_weight, out_weight, layout
):
    local_rows, model_width = fixed_point.shape
    head_width = query_weight.shape[1]
    head_count = head_width // HEAD_DIM
    seq_tokens = local_rows * lax.axis_size("tensor")
    seq_length = seq_tokens * lax.axis_size("seq")
    seq_index = lax.axis_index("seq")
    score_scale = HEAD_DIM ** (-0.5)
    contract_last = (((1,), (1,)), ((), ()))
    head_shape = (seq_tokens, head_count, HEAD_DIM)
    point = fixed_point.astype(jnp.float32)
    inv_rms = lax.rsqrt(jnp.mean(point * point, axis=1, keepdims=True) + EPS)
    scaled = point * inv_rms
    normed = (norm_gain * scaled).astype(jnp.bfloat16)
    project_piece = lax.all_gather(normed, "tensor", axis=0, tiled=True)
    projected = jnp.concatenate(
        [
            jnp.dot(project_piece, query_weight, preferred_element_type=jnp.float32),
            jnp.dot(project_piece, key_weight, preferred_element_type=jnp.float32),
            jnp.dot(project_piece, value_weight, preferred_element_type=jnp.float32),
        ],
        axis=1,
    )
    positions = seq_index * seq_tokens + jnp.arange(seq_tokens, dtype=jnp.int32)
    cosine, sine = rope_tables(positions)
    queries = rotate(projected[:, :head_width].reshape(head_shape), cosine, sine).astype(
        jnp.bfloat16
    )
    keys = rotate(
        projected[:, head_width : 2 * head_width].reshape(head_shape), cosine, sine
    ).astype(jnp.bfloat16)
    values = projected[:, 2 * head_width :].reshape(head_shape).astype(jnp.bfloat16)
    block_rows = seq_tokens // BLK
    block_count = seq_length // BLK
    first_block = seq_index * block_rows
    key_positions = jnp.arange(seq_length, dtype=jnp.int32)
    chosen_rows = (
        lax.dynamic_slice(layout, (first_block, jnp.int32(0)), (block_rows, block_count)) > 0
    )
    allowed = pair_mask(positions, key_positions, expand_blocks(chosen_rows))
    keys_all, values_all = (
        lax.all_gather(keys, "seq", axis=0, tiled=True),
        lax.all_gather(values, "seq", axis=0, tiled=True),
    )
    scores = (
        jnp.einsum("qhd,khd->hqk", queries, keys_all, preferred_element_type=jnp.float32)
        * score_scale
    )
    scores = jnp.where(allowed[None], scores, MASKED)
    log_norm = jax.nn.logsumexp(scores, axis=2, keepdims=True)
    probs = jnp.exp(scores - log_norm)
    probs_low = probs.astype(jnp.bfloat16)
    attended = jnp.einsum(
        "hqk,khd->qhd", probs_low, values_all, preferred_element_type=jnp.float32
    ).astype(jnp.bfloat16)
    cotangent = incoming.astype(jnp.float32)
    adjoint = cotangent
    gain_grad = jnp.zeros((model_width,), jnp.float32)
    for term_index in range(ITERS):
        grad_out = lax.dot_general(
            lax.all_gather(cotangent.astype(jnp.bfloat16), "tensor", axis=0, tiled=True),
            out_weight,
            contract_last,
            preferred_element_type=jnp.float32,
        )
        grad_low = grad_out.astype(jnp.bfloat16).reshape(head_shape)
        delta = jnp.sum(grad_low.astype(jnp.float32) * attended.astype(jnp.float32), axis=2)
        grad_probs = jnp.einsum(
            "qhd,khd->hqk", grad_low, values_all, preferred_element_type=jnp.float32
        )
        grad_scores = (probs * (grad_probs - delta.T[:, :, None])).astype(jnp.bfloat16)
        grad_query = (
            jnp.einsum("hqk,khd->qhd", grad_scores, keys_all, preferred_element_type=jnp.float32)
            * score_scale
        )
        key_part = (
            jnp.einsum("hqk,qhd->khd", grad_scores, queries, preferred_element_type=jnp.float32)
            * score_scale
        )
        value_part = jnp.einsum(
            "hqk,qhd->khd", probs_low, grad_low, preferred_element_type=jnp.float32
        )
        key_grads = lax.psum_scatter(
            jnp.concatenate(
                [
                    key_part.reshape(seq_tokens * lax.axis_size("seq"), head_width),
                    value_part.reshape(seq_tokens * lax.axis_size("seq"), head_width),
                ],
                axis=1,
            ).astype(jnp.bfloat16),
            "seq",
            scatter_dimension=0,
            tiled=True,
        ).astype(jnp.float32)
        grad_key = key_grads[:, :head_width].reshape(head_shape)
        grad_value = key_grads[:, head_width:].reshape(head_shape)
        query_low = (
            rotate_back(grad_query, cosine, sine)
            .astype(jnp.bfloat16)
            .reshape(seq_tokens, head_width)
        )
        key_low = (
            rotate_back(grad_key, cosine, sine).astype(jnp.bfloat16).reshape(seq_tokens, head_width)
        )
        value_low = grad_value.astype(jnp.bfloat16).reshape(seq_tokens, head_width)
        total = lax.dot_general(
            query_low, query_weight, contract_last, preferred_element_type=jnp.float32
        )
        total = total + lax.dot_general(
            key_low, key_weight, contract_last, preferred_element_type=jnp.float32
        )
        total = total + lax.dot_general(
            value_low, value_weight, contract_last, preferred_element_type=jnp.float32
        )
        grad_normed = lax.psum_scatter(
            total.astype(jnp.bfloat16), "tensor", scatter_dimension=0, tiled=True
        ).astype(jnp.float32)
        gain_term = jnp.sum(grad_normed * scaled, axis=0)
        gain_grad = gain_grad + lax.psum(gain_term, ("seq", "tensor"))
        weighted = norm_gain * grad_normed
        inner = jnp.sum(weighted * scaled, axis=1, keepdims=True)
        cotangent = inv_rms * (weighted - scaled * (inner / model_width))
        adjoint = adjoint + cotangent
    return (adjoint, gain_grad * seq_length ** (-0.5))


CHUNKS = 4
MESH = pl.DeviceIdType.MESH


def numpy_tables(length):
    freq = np.float32(THETA) ** (-np.arange(0, HEAD_DIM, 2, dtype=np.float32) / np.float32(HEAD_DIM))
    angle = np.arange(length, dtype=np.float32)[:, None] * freq.astype(np.float32)[None, :]
    cosine = np.cos(angle.astype(np.float64)).astype(np.float32)
    sine = np.sin(angle.astype(np.float64)).astype(np.float32)
    return np.concatenate([cosine, cosine], axis=1), np.concatenate([-sine, sine], axis=1)


def product(left, right, left_dim, right_dim):
    return lax.dot_general(
        left, right, (((left_dim,), (right_dim,)), ((), ())), preferred_element_type=jnp.float32
    )


def flipped(index, mask, bits):
    result = 0
    for bit in range(bits):
        here = lax.rem(lax.div(index, 1 << bit), 2)
        result = result + (1 << bit) * ((1 - here) if (mask >> bit) & 1 else here)
    return result


def window(index, size):
    return pl.ds(pl.multiple_of(index * size, size), size)


def fused_body(
    fixed_point, incoming, norm_gain, query_weight, key_weight, value_weight, out_weight, layout
):
    rows, width = fixed_point.shape
    tensor_count = lax.axis_size("tensor")
    seq_count = lax.axis_size("seq")
    chips = tensor_count // 2
    bits = seq_count.bit_length() - 1
    head_width = query_weight.shape[1]
    tokens = rows * tensor_count
    length = tokens * seq_count
    blocks = layout.shape[0]
    part = width // CHUNKS
    score_scale = HEAD_DIM ** (-0.5)
    gain_rows = width // HEAD_DIM
    gain_part = gain_rows // CHUNKS
    cosine, sine = numpy_tables(length)
    order = list(range(seq_count - 1, 0, -1))
    low, full = jnp.bfloat16, jnp.float32
    dma = pltpu.SemaphoreType.DMA
    hops = 2 * chips - 1
    scratch = {
        "wq": pltpu.VMEM((width, head_width), low),
        "wk": pltpu.VMEM((width, head_width), low),
        "wv": pltpu.VMEM((width, head_width), low),
        "wo": pltpu.VMEM((head_width, width), low),
        "point": pltpu.VMEM((rows, width), low),
        "gain": pltpu.VMEM((1, width), full),
        "layout": pltpu.VMEM(layout.shape, jnp.int32),
        "cosine": pltpu.VMEM((length, HEAD_DIM), full),
        "sine": pltpu.VMEM((length, HEAD_DIM), full),
        "bias": pltpu.VMEM((blocks, length), full),
        "scaled": pltpu.VMEM((rows, width), full),
        "pieces": pltpu.VMEM((1 + ITERS, tokens, width), low),
        "acc": pltpu.VMEM((4, tokens, head_width), full),
        "heads_out": pltpu.VMEM((3 + ITERS, seq_count, tokens, HEAD_DIM), low),
        "heads_in": pltpu.VMEM((3 + ITERS, length, HEAD_DIM), low),
        "probs": pltpu.VMEM((length, length), low),
        "key_acc": pltpu.VMEM((length, HEAD_DIM), full),
        "value_acc": pltpu.VMEM((length, HEAD_DIM), full),
        "grads_out": pltpu.VMEM((3 * ITERS, length, HEAD_DIM), low),
        "grads_in": pltpu.VMEM((3 * ITERS, tokens, head_width), low),
        "total": pltpu.VMEM((tokens, width), full),
        "hand_out": pltpu.VMEM((ITERS * chips, rows, width), low),
        "hand_in": pltpu.VMEM((ITERS * chips, rows, width), low),
        "far_out": pltpu.VMEM((ITERS * chips, rows, width), low),
        "far_in": pltpu.VMEM((ITERS * chips, rows, width), low),
        "normed_grad": pltpu.VMEM((rows, width), full),
        "adjoint": pltpu.VMEM((rows, width), full),
        "gain_sum": pltpu.VMEM((1, width), full),
        "gain_own": pltpu.VMEM((gain_rows, HEAD_DIM), full),
        "gain_near": pltpu.VMEM((tensor_count, gain_rows, HEAD_DIM), full),
        "gain_mid": pltpu.VMEM((gain_rows, HEAD_DIM), full),
        "gain_far": pltpu.VMEM((seq_count, gain_rows, HEAD_DIM), full),
        "gain_out": pltpu.VMEM((gain_rows, HEAD_DIM), full),
        "load_sem": dma((7,)),
        "weight_sem": dma((4, CHUNKS)),
        "gather_send": dma((1 + ITERS, CHUNKS, hops)),
        "gather_recv": dma((1 + ITERS, CHUNKS, hops)),
        "heads_send": dma((3 + ITERS, seq_count)),
        "heads_recv": dma((3 + ITERS, seq_count)),
        "grads_send": dma((3 * ITERS, seq_count)),
        "grads_recv": dma((3 * ITERS, seq_count)),
        "hand_send": dma((ITERS * chips, CHUNKS)),
        "hand_recv": dma((ITERS * chips, CHUNKS)),
        "far_send": dma((ITERS * chips, CHUNKS)),
        "far_recv": dma((ITERS * chips, CHUNKS)),
        "near_send": dma((tensor_count, CHUNKS)),
        "near_recv": dma((tensor_count, CHUNKS)),
        "wide_send": dma((seq_count, CHUNKS)),
        "wide_recv": dma((seq_count, CHUNKS)),
    }

    def kernel(*refs):
        point_hbm, incoming_hbm, gain_hbm, wq_hbm, wk_hbm, wv_hbm, wo_hbm = refs[:7]
        layout_hbm, cosine_hbm, sine_hbm, adjoint_hbm, gain_out_hbm = refs[7:12]
        r = types.SimpleNamespace(**dict(zip(scratch, refs[12:])))
        me_seq = lax.axis_index("seq")
        me = lax.axis_index("tensor")
        core = lax.rem(me, 2)
        chip = lax.div(me, 2)
        partner = me + 1 - 2 * core
        own_rows = window(me, rows)
        own_tokens = window(me_seq, tokens)
        own_columns = window(me_seq, HEAD_DIM)

        barrier = pltpu.get_barrier_semaphore()
        for step in range(1, tensor_count):
            pl.semaphore_signal(
                barrier,
                inc=1,
                device_id={"tensor": lax.rem(me + step, tensor_count)},
                device_id_type=MESH,
            )
        for mask in order:
            pl.semaphore_signal(
                barrier,
                inc=1,
                device_id={"seq": flipped(me_seq, mask, bits)},
                device_id_type=MESH,
            )

        def load(index, source, target):
            return pltpu.make_async_copy(source, target, r.load_sem.at[index])

        loads = [
            load(0, point_hbm, r.point),
            load(1, gain_hbm, r.gain),
            load(2, incoming_hbm, r.pieces.at[1, own_rows, :]),
            load(3, layout_hbm, r.layout),
            load(4, cosine_hbm, r.cosine),
            load(5, sine_hbm, r.sine),
        ]
        for copy in loads:
            copy.start()

        def weight_load(item, chunk):
            source = (wq_hbm, wk_hbm, wv_hbm, wo_hbm)[item]
            target = (r.wq, r.wk, r.wv, r.wo)[item]
            place = window(chunk, part)
            if item < 3:
                source, target = source.at[place, :], target.at[place, :]
            else:
                source, target = source.at[:, place], target.at[:, place]
            return pltpu.make_async_copy(source, target, r.weight_sem.at[item, chunk])

        for chunk in range(CHUNKS):
            for item in range(3):
                weight_load(item, chunk).start()
        for chunk in range(CHUNKS):
            weight_load(3, chunk).start()

        def remote(source, target, send, recv, axis, peer):
            return pltpu.make_async_remote_copy(
                src_ref=source,
                dst_ref=target,
                send_sem=send,
                recv_sem=recv,
                device_id={axis: peer},
                device_id_type=MESH,
            )

        def gather_copy(item, chunk, slot, origin, peer):
            block = r.pieces.at[item, window(origin, rows), window(chunk, part)]
            return remote(
                block,
                block,
                r.gather_send.at[item, chunk, slot],
                r.gather_recv.at[item, chunk, slot],
                "tensor",
                peer,
            )

        def gather_far(item, chunk, step):
            peer = 2 * lax.rem(chip + step, chips) + core
            return gather_copy(item, chunk, step, me, peer)

        def gather_near(item, chunk):
            return gather_copy(item, chunk, 0, me, partner)

        def gather_pass(item, chunk, step):
            origin = 2 * lax.rem(chip + chips - step, chips) + core
            return gather_copy(item, chunk, chips - 1 + step, origin, partner)

        def gather_start(item):
            for chunk in range(CHUNKS):
                for step in range(1, chips):
                    gather_far(item, chunk, step).start()
                gather_near(item, chunk).start()

        def gather_relay(item, chunk):
            for step in range(1, chips):
                gather_far(item, chunk, step).wait_recv()
                gather_pass(item, chunk, step).start()

        def gather_ready(item, chunk):
            gather_near(item, chunk).wait_recv()
            for step in range(1, chips):
                gather_pass(item, chunk, step).wait_recv()

        def gather_drain(item):
            def drain(chunk, carry):
                gather_near(item, chunk).wait_send()
                for step in range(1, chips):
                    gather_far(item, chunk, step).wait_send()
                    gather_pass(item, chunk, step).wait_send()
                return carry

            lax.fori_loop(0, CHUNKS, drain, 0)

        def gather_each(item, use):
            gather_relay(item, 0)

            def body(chunk, carry):
                @pl.when(chunk + 1 < CHUNKS)
                def _():
                    gather_relay(item, chunk + 1)

                gather_ready(item, chunk)
                use(chunk)
                return carry

            lax.fori_loop(0, CHUNKS, body, 0)

        def heads_copy(item, mask):
            return remote(
                r.heads_out.at[item, mask],
                r.heads_in.at[item, own_tokens, :],
                r.heads_send.at[item, mask],
                r.heads_recv.at[item, mask],
                "seq",
                flipped(me_seq, mask, bits),
            )

        def heads_start(item, slot, turn):
            for mask in order + [0]:
                columns = window(flipped(me_seq, mask, bits), HEAD_DIM)
                values = r.acc[slot, :, columns]
                if turn:
                    values = (
                        values * r.cosine[own_tokens, :]
                        + pltpu.roll(values, HEAD_DIM // 2, 1) * r.sine[own_tokens, :]
                    )
                if mask:
                    r.heads_out[item, mask] = values.astype(low)
                else:
                    r.heads_in[item, own_tokens, :] = values.astype(low)
            for mask in order:
                heads_copy(item, mask).start()

        def heads_ready(item):
            for mask in order:
                heads_copy(item, mask).wait_recv()

        def grads_copy(item, mask):
            peer = flipped(me_seq, mask, bits)
            return remote(
                r.grads_out.at[item, window(peer, tokens), :],
                r.grads_in.at[item, :, own_columns],
                r.grads_send.at[item, mask],
                r.grads_recv.at[item, mask],
                "seq",
                peer,
            )

        def grads_start(item):
            for mask in order:
                grads_copy(item, mask).start()
            r.grads_in[item, :, own_columns] = r.grads_out[item, own_tokens, :]

        def grads_ready(item):
            for mask in order:
                grads_copy(item, mask).wait_recv()

        def hand_copy(term, step, chunk):
            place = window(chunk, part)
            item = term * chips + step
            return remote(
                r.hand_out.at[item, :, place],
                r.hand_in.at[item, :, place],
                r.hand_send.at[item, chunk],
                r.hand_recv.at[item, chunk],
                "tensor",
                partner,
            )

        def far_copy(term, step, chunk):
            place = window(chunk, part)
            item = term * chips + step
            return remote(
                r.far_out.at[item, :, place],
                r.far_in.at[item, :, place],
                r.far_send.at[item, chunk],
                r.far_recv.at[item, chunk],
                "tensor",
                2 * lax.rem(chip + step, chips) + core,
            )

        def near_copy(step, chunk):
            place = window(chunk, gain_part)
            return remote(
                r.gain_own.at[place, :],
                r.gain_near.at[step, place, :],
                r.near_send.at[step, chunk],
                r.near_recv.at[step, chunk],
                "tensor",
                lax.rem(me + step, tensor_count),
            )

        def wide_copy(mask, chunk):
            place = window(chunk, gain_part)
            return remote(
                r.gain_mid.at[place, :],
                r.gain_far.at[mask, place, :],
                r.wide_send.at[mask, chunk],
                r.wide_recv.at[mask, chunk],
                "seq",
                flipped(me_seq, mask, bits),
            )

        loads[0].wait()
        loads[1].wait()
        point = r.point[...].astype(full)
        inv_rms = lax.rsqrt(jnp.mean(point * point, axis=1, keepdims=True) + EPS)
        r.scaled[...] = point * inv_rms
        r.pieces[0, own_rows, :] = (r.gain[...] * r.scaled[...]).astype(low)
        loads[2].wait()
        pl.semaphore_wait(barrier, tensor_count - 1 + seq_count - 1)
        gather_start(0)
        gather_start(1)

        loads[3].wait()
        spread = (
            lax.broadcasted_iota(jnp.int32, (blocks, length), 1) // BLK
            == lax.broadcasted_iota(jnp.int32, (blocks, length), 0)
        )
        chosen = product(
            jnp.where(r.layout[...] > 0, 1.0, 0.0).astype(low),
            jnp.where(spread, 1.0, 0.0).astype(low),
            1,
            0,
        )
        earlier = (
            lax.broadcasted_iota(jnp.int32, (blocks, length), 1) // BLK
            < lax.broadcasted_iota(jnp.int32, (blocks, length), 0)
        )
        r.bias[...] = jnp.where(earlier & (chosen > 0.5), 0.0, MASKED)
        r.acc[...] = jnp.zeros(r.acc.shape, full)

        def project(chunk):
            place = window(chunk, part)
            for item, weight in enumerate((r.wq, r.wk, r.wv)):
                weight_load(item, chunk).wait()
                r.acc[item] += product(r.pieces[0, :, place], weight[place, :], 1, 0)

        gather_each(0, project)
        loads[4].wait()
        loads[5].wait()
        heads_start(0, 0, True)
        heads_start(1, 1, True)
        heads_start(2, 2, False)

        def pull(item):
            def use(chunk):
                if item == 1:
                    weight_load(3, chunk).wait()
                place = window(chunk, part)
                r.acc[3] += product(r.pieces[item, :, place], r.wo[:, place], 1, 1)

            return use

        gather_each(1, pull(1))
        heads_start(3, 3, False)

        group = 2 if seq_count % 2 == 0 else 1
        heads_ready(0)
        heads_ready(1)
        sub = tokens // BLK

        def forward(base):
            span = (base + group) * tokens

            def body(step, carry):
                place = window(base + step, tokens)
                scores = product(r.heads_in[0, place, :], r.heads_in[1, :span, :], 1, 1) * score_scale
                query_at = (base + step) * tokens + lax.broadcasted_iota(jnp.int32, (tokens, span), 0)
                key_at = lax.broadcasted_iota(jnp.int32, (tokens, span), 1)
                same = (query_at // BLK == key_at // BLK) & (key_at <= query_at)
                bias = jnp.concatenate(
                    [
                        jnp.broadcast_to(r.bias[pl.ds((base + step) * sub + line, 1), :span], (BLK, span))
                        for line in range(sub)
                    ],
                    axis=0,
                )
                scores = scores + jnp.where(same, 0.0, bias)
                top = jnp.max(scores, axis=1, keepdims=True)
                weight = jnp.exp(scores - top)
                r.probs[place, :span] = (weight / jnp.sum(weight, axis=1, keepdims=True)).astype(low)
                return carry

            lax.fori_loop(0, group, body, 0)

        for base in range(0, seq_count, group):
            forward(base)

        def turned_back(values, place):
            return (
                values * r.cosine[place, :]
                - pltpu.roll(values, HEAD_DIM // 2, 1) * r.sine[place, :]
            ).astype(low)

        def backward(term):
            r.key_acc[...] = jnp.zeros(r.key_acc.shape, full)
            r.value_acc[...] = jnp.zeros(r.value_acc.shape, full)

            def at(base):
                span = (base + group) * tokens

                def body(step, carry):
                    place = window(base + group - 1 - step, tokens)
                    probs = r.probs[place, :span]
                    grad_low = r.heads_in[3 + term, place, :]
                    grad_probs = product(grad_low, r.heads_in[2, :span, :], 1, 1)
                    wide = probs.astype(full)
                    delta = jnp.sum(wide * grad_probs, axis=1, keepdims=True)
                    grad_scores = (wide * (grad_probs - delta)).astype(low)
                    grad_query = product(grad_scores, r.heads_in[1, :span, :], 1, 0) * score_scale
                    r.grads_out[3 * term, place, :] = turned_back(grad_query, place)
                    r.key_acc[:span, :] += product(grad_scores, r.heads_in[0, place, :], 0, 0)
                    r.value_acc[:span, :] += product(probs, grad_low, 0, 0)
                    return carry

                lax.fori_loop(0, group, body, 0)

            for base in reversed(range(0, seq_count, group)):
                at(base)
            r.grads_out[3 * term + 2] = r.value_acc[...].astype(low)
            grads_start(3 * term + 2)
            r.grads_out[3 * term + 1] = turned_back(r.key_acc[...] * score_scale, slice(None))
            grads_start(3 * term + 1)
            grads_start(3 * term)

        def hand_on(term, chunk):
            place = window(chunk, part)
            for step in range(chips):
                hand_copy(term, step, chunk).wait_recv()
                owner = 2 * lax.rem(chip + step, chips) + core
                pair = r.total[window(owner, rows), place] + r.hand_in[
                    term * chips + step, :, place
                ].astype(full)
                if step:
                    r.far_out[term * chips + step, :, place] = pair.astype(low)
                    far_copy(term, step, chunk).start()
                else:
                    r.normed_grad[:, place] = pair

        def push(term):
            for item, weight in ((2, r.wv), (1, r.wk)):
                grads_ready(3 * term + item)

                def body(chunk, carry):
                    place = window(chunk, part)
                    value = product(r.grads_in[3 * term + item], weight[place, :], 1, 1)
                    if item == 1:
                        value = value + r.total[:, place]
                    r.total[:, place] = value
                    return carry

                lax.fori_loop(0, CHUNKS, body, 0)
            grads_ready(3 * term)

            def last(chunk, carry):
                place = window(chunk, part)
                r.total[:, place] += product(r.grads_in[3 * term], r.wq[place, :], 1, 1)
                for step in range(chips):
                    other = 2 * lax.rem(chip + step, chips) + 1 - core
                    r.hand_out[term * chips + step, :, place] = r.total[
                        window(other, rows), place
                    ].astype(low)
                for step in range(chips):
                    hand_copy(term, step, chunk).start()

                @pl.when(chunk > 0)
                def _():
                    hand_on(term, chunk - 1)

                return carry

            lax.fori_loop(0, CHUNKS, last, 0)
            hand_on(term, CHUNKS - 1)

        def near_sum(chunk):
            for step in range(1, tensor_count):
                near_copy(step, chunk).wait_recv()
            place = window(chunk, gain_part)
            value = r.gain_own[place, :]
            for step in range(1, tensor_count):
                value = value + r.gain_near[step, place, :]
            r.gain_mid[place, :] = value
            for mask in order:
                wide_copy(mask, chunk).start()

        for term in range(ITERS):
            if term:
                r.acc[3] = jnp.zeros((tokens, head_width), full)
                gather_start(1 + term)
                gather_each(1 + term, pull(1 + term))
                heads_start(3 + term, 3, False)
            else:
                heads_ready(2)
            heads_ready(3 + term)
            backward(term)
            push(term)
            final = term == ITERS - 1
            for chunk in range(CHUNKS):
                place = slice(chunk * part, (chunk + 1) * part)
                value = r.normed_grad[:, place]
                for step in range(1, chips):
                    far_copy(term, step, chunk).wait_recv()
                    value = value + r.far_in[term * chips + step, :, place].astype(full)
                r.normed_grad[:, place] = value
                gain_term = jnp.sum(value * r.scaled[:, place], axis=0, keepdims=True)
                if term:
                    gain_term = gain_term + r.gain_sum[:, place]
                if not final:
                    r.gain_sum[:, place] = gain_term
                    continue
                for line in range(gain_part):
                    r.gain_own[chunk * gain_part + line : chunk * gain_part + line + 1, :] = gain_term[
                        :, line * HEAD_DIM : (line + 1) * HEAD_DIM
                    ]
                for step in range(1, tensor_count):
                    near_copy(step, chunk).start()
                if chunk:
                    near_sum(chunk - 1)
            weighted = r.gain[...] * r.normed_grad[...]
            inner = jnp.sum(weighted * r.scaled[...], axis=1, keepdims=True)
            cotangent = inv_rms * (weighted - r.scaled[...] * (inner / width))
            if term == 0:
                r.adjoint[...] = r.pieces[1, own_rows, :].astype(full) + cotangent
            else:
                r.adjoint[...] += cotangent
            if not final:
                r.pieces[2 + term, own_rows, :] = cotangent.astype(low)

        out_copy = load(6, r.adjoint, adjoint_hbm)
        out_copy.start()
        near_sum(CHUNKS - 1)
        for item in range(1 + ITERS):
            gather_drain(item)
        for item in range(3 + ITERS):
            for mask in order:
                heads_copy(item, mask).wait_send()
        for item in range(3 * ITERS):
            for mask in order:
                grads_copy(item, mask).wait_send()
        for chunk in range(CHUNKS):
            for term in range(ITERS):
                for step in range(chips):
                    hand_copy(term, step, chunk).wait_send()
                    if step:
                        far_copy(term, step, chunk).wait_send()
            for step in range(1, tensor_count):
                near_copy(step, chunk).wait_send()
        for chunk in range(CHUNKS):
            for mask in order:
                wide_copy(mask, chunk).wait()
        value = r.gain_mid[...]
        for mask in order:
            value = value + r.gain_far[mask]
        r.gain_out[...] = value * length ** (-0.5)
        out_copy.wait()
        gain_copy = load(0, r.gain_out, gain_out_hbm)
        gain_copy.start()
        gain_copy.wait()

    anywhere = pl.BlockSpec(memory_space=pl.ANY)
    adjoint, gain_grad = pl.pallas_call(
        kernel,
        out_shape=[
            jax.ShapeDtypeStruct((rows, width), full),
            jax.ShapeDtypeStruct((gain_rows, HEAD_DIM), full),
        ],
        in_specs=[anywhere] * 10,
        out_specs=[anywhere] * 2,
        scratch_shapes=list(scratch.values()),
        compiler_params=pltpu.CompilerParams(
            collective_id=0, has_side_effects=True, vmem_limit_bytes=67043328
        ),
    )(
        fixed_point,
        incoming,
        norm_gain.reshape(1, width),
        query_weight,
        key_weight,
        value_weight,
        out_weight,
        layout,
        jnp.asarray(cosine),
        jnp.asarray(sine),
    )
    return adjoint, gain_grad.reshape(width)


def solution(mesh):
    in_specs = (
        P(("seq", "tensor"), None),
        P(("seq", "tensor"), None),
        P(),
        P(None, "tensor"),
        P(None, "tensor"),
        P(None, "tensor"),
        P("tensor", None),
        P(),
    )
    out_specs = (P(("seq", "tensor"), None), P())
    seq, tensor = mesh.shape["seq"], mesh.shape["tensor"]

    def body(*arrays):
        heads = arrays[3].shape[1] * tensor // HEAD_DIM
        tokens = arrays[0].shape[0] * tensor
        fits = (
            tensor % 2 == 0
            and seq & (seq - 1) == 0
            and heads == seq * tensor
            and tokens % 128 == 0
            and arrays[0].shape[0] % 16 == 0
            and arrays[0].shape[1] % (8 * HEAD_DIM * CHUNKS) == 0
        )
        return (fused_body if fits else ring_body)(*arrays)

    return jax.shard_map(body, mesh=mesh, in_specs=in_specs, out_specs=out_specs, check_vma=False)
```

```python
import types

import jax
import jax.numpy as jnp
import numpy as np
from jax import lax
from jax.experimental import pallas as pl
from jax.experimental.pallas import tpu as pltpu
from jax.sharding import PartitionSpec as P

HEAD_DIM = 128
BLK = 64
ITERS = 2


EPS = 1e-05
THETA = 10000.0
MASKED = -1e30


def rope_tables(positions):
    freq = THETA ** (-jnp.arange(0, HEAD_DIM, 2, dtype=jnp.float32) / HEAD_DIM)
    angle = positions.astype(jnp.float32)[:, None] * freq[None, :]
    cosine = jnp.concatenate([jnp.cos(angle), jnp.cos(angle)], axis=1)[:, None, :]
    sine = jnp.concatenate([jnp.sin(angle), jnp.sin(angle)], axis=1)[:, None, :]
    return (cosine, sine)


def rotate(values, cosine, sine):
    half = HEAD_DIM // 2
    turned = jnp.concatenate([-values[..., half:], values[..., :half]], axis=-1)
    return values * cosine + turned * sine


def rotate_back(values, cosine, sine):
    half = HEAD_DIM // 2
    weighted = values * sine
    turned = jnp.concatenate([weighted[..., half:], -weighted[..., :half]], axis=-1)
    return values * cosine + turned


def expand_blocks(chosen):
    return jnp.repeat(jnp.repeat(chosen, BLK, axis=0), BLK, axis=1)


def pair_mask(query_pos, key_pos, chosen):
    query_block = (query_pos // BLK)[:, None]
    key_block = (key_pos // BLK)[None, :]
    earlier = (key_block < query_block) & chosen
    same = (key_block == query_block) & (key_pos[None, :] <= query_pos[:, None])
    return earlier | same


def ring_body(
    fixed_point, incoming, norm_gain, query_weight, key_weight, value_weight, out_weight, layout
):
    local_rows, model_width = fixed_point.shape
    head_width = query_weight.shape[1]
    head_count = head_width // HEAD_DIM
    seq_tokens = local_rows * lax.axis_size("tensor")
    seq_length = seq_tokens * lax.axis_size("seq")
    seq_index = lax.axis_index("seq")
    score_scale = HEAD_DIM ** (-0.5)
    contract_last = (((1,), (1,)), ((), ()))
    head_shape = (seq_tokens, head_count, HEAD_DIM)
    point = fixed_point.astype(jnp.float32)
    inv_rms = lax.rsqrt(jnp.mean(point * point, axis=1, keepdims=True) + EPS)
    scaled = point * inv_rms
    normed = (norm_gain * scaled).astype(jnp.bfloat16)
    project_piece = lax.all_gather(normed, "tensor", axis=0, tiled=True)
    projected = jnp.concatenate(
        [
            jnp.dot(project_piece, query_weight, preferred_element_type=jnp.float32),
            jnp.dot(project_piece, key_weight, preferred_element_type=jnp.float32),
            jnp.dot(project_piece, value_weight, preferred_element_type=jnp.float32),
        ],
        axis=1,
    )
    positions = seq_index * seq_tokens + jnp.arange(seq_tokens, dtype=jnp.int32)
    cosine, sine = rope_tables(positions)
    queries = rotate(projected[:, :head_width].reshape(head_shape), cosine, sine).astype(
        jnp.bfloat16
    )
    keys = rotate(
        projected[:, head_width : 2 * head_width].reshape(head_shape), cosine, sine
    ).astype(jnp.bfloat16)
    values = projected[:, 2 * head_width :].reshape(head_shape).astype(jnp.bfloat16)
    block_rows = seq_tokens // BLK
    block_count = seq_length // BLK
    first_block = seq_index * block_rows
    key_positions = jnp.arange(seq_length, dtype=jnp.int32)
    chosen_rows = (
        lax.dynamic_slice(layout, (first_block, jnp.int32(0)), (block_rows, block_count)) > 0
    )
    allowed = pair_mask(positions, key_positions, expand_blocks(chosen_rows))
    keys_all, values_all = (
        lax.all_gather(keys, "seq", axis=0, tiled=True),
        lax.all_gather(values, "seq", axis=0, tiled=True),
    )
    scores = (
        jnp.einsum("qhd,khd->hqk", queries, keys_all, preferred_element_type=jnp.float32)
        * score_scale
    )
    scores = jnp.where(allowed[None], scores, MASKED)
    log_norm = jax.nn.logsumexp(scores, axis=2, keepdims=True)
    probs = jnp.exp(scores - log_norm)
    probs_low = probs.astype(jnp.bfloat16)
    attended = jnp.einsum(
        "hqk,khd->qhd", probs_low, values_all, preferred_element_type=jnp.float32
    ).astype(jnp.bfloat16)
    cotangent = incoming.astype(jnp.float32)
    adjoint = cotangent
    gain_grad = jnp.zeros((model_width,), jnp.float32)
    for term_index in range(ITERS):
        grad_out = lax.dot_general(
            lax.all_gather(cotangent.astype(jnp.bfloat16), "tensor", axis=0, tiled=True),
            out_weight,
            contract_last,
            preferred_element_type=jnp.float32,
        )
        grad_low = grad_out.astype(jnp.bfloat16).reshape(head_shape)
        delta = jnp.sum(grad_low.astype(jnp.float32) * attended.astype(jnp.float32), axis=2)
        grad_probs = jnp.einsum(
            "qhd,khd->hqk", grad_low, values_all, preferred_element_type=jnp.float32
        )
        grad_scores = (probs * (grad_probs - delta.T[:, :, None])).astype(jnp.bfloat16)
        grad_query = (
            jnp.einsum("hqk,khd->qhd", grad_scores, keys_all, preferred_element_type=jnp.float32)
            * score_scale
        )
        key_part = (
            jnp.einsum("hqk,qhd->khd", grad_scores, queries, preferred_element_type=jnp.float32)
            * score_scale
        )
        value_part = jnp.einsum(
            "hqk,qhd->khd", probs_low, grad_low, preferred_element_type=jnp.float32
        )
        key_grads = lax.psum_scatter(
            jnp.concatenate(
                [
                    key_part.reshape(seq_tokens * lax.axis_size("seq"), head_width),
                    value_part.reshape(seq_tokens * lax.axis_size("seq"), head_width),
                ],
                axis=1,
            ).astype(jnp.bfloat16),
            "seq",
            scatter_dimension=0,
            tiled=True,
        ).astype(jnp.float32)
        grad_key = key_grads[:, :head_width].reshape(head_shape)
        grad_value = key_grads[:, head_width:].reshape(head_shape)
        query_low = (
            rotate_back(grad_query, cosine, sine)
            .astype(jnp.bfloat16)
            .reshape(seq_tokens, head_width)
        )
        key_low = (
            rotate_back(grad_key, cosine, sine).astype(jnp.bfloat16).reshape(seq_tokens, head_width)
        )
        value_low = grad_value.astype(jnp.bfloat16).reshape(seq_tokens, head_width)
        total = lax.dot_general(
            query_low, query_weight, contract_last, preferred_element_type=jnp.float32
        )
        total = total + lax.dot_general(
            key_low, key_weight, contract_last, preferred_element_type=jnp.float32
        )
        total = total + lax.dot_general(
            value_low, value_weight, contract_last, preferred_element_type=jnp.float32
        )
        grad_normed = lax.psum_scatter(
            total.astype(jnp.bfloat16), "tensor", scatter_dimension=0, tiled=True
        ).astype(jnp.float32)
        gain_term = jnp.sum(grad_normed * scaled, axis=0)
        gain_grad = gain_grad + lax.psum(gain_term, ("seq", "tensor"))
        weighted = norm_gain * grad_normed
        inner = jnp.sum(weighted * scaled, axis=1, keepdims=True)
        cotangent = inv_rms * (weighted - scaled * (inner / model_width))
        adjoint = adjoint + cotangent
    return (adjoint, gain_grad * seq_length ** (-0.5))


CHUNKS = 4
MESH = pl.DeviceIdType.MESH


def numpy_tables(length):
    freq = np.float32(THETA) ** (-np.arange(0, HEAD_DIM, 2, dtype=np.float32) / np.float32(HEAD_DIM))
    angle = np.arange(length, dtype=np.float32)[:, None] * freq.astype(np.float32)[None, :]
    cosine = np.cos(angle.astype(np.float64)).astype(np.float32)
    sine = np.sin(angle.astype(np.float64)).astype(np.float32)
    return np.concatenate([cosine, cosine], axis=1), np.concatenate([-sine, sine], axis=1)


def product(left, right, left_dim, right_dim):
    return lax.dot_general(
        left, right, (((left_dim,), (right_dim,)), ((), ())), preferred_element_type=jnp.float32
    )


def flipped(index, mask, bits):
    result = 0
    for bit in range(bits):
        here = lax.rem(lax.div(index, 1 << bit), 2)
        result = result + (1 << bit) * ((1 - here) if (mask >> bit) & 1 else here)
    return result


def window(index, size):
    return pl.ds(pl.multiple_of(index * size, size), size)


def fused_body(
    fixed_point, incoming, norm_gain, query_weight, key_weight, value_weight, out_weight, layout
):
    rows, width = fixed_point.shape
    tensor_count = lax.axis_size("tensor")
    seq_count = lax.axis_size("seq")
    chips = tensor_count // 2
    bits = seq_count.bit_length() - 1
    head_width = query_weight.shape[1]
    tokens = rows * tensor_count
    length = tokens * seq_count
    blocks = layout.shape[0]
    part = width // CHUNKS
    score_scale = HEAD_DIM ** (-0.5)
    gain_rows = width // HEAD_DIM
    gain_part = gain_rows // CHUNKS
    cosine, sine = numpy_tables(length)
    order = list(range(seq_count - 1, 0, -1))
    low, full = jnp.bfloat16, jnp.float32
    dma = pltpu.SemaphoreType.DMA
    scratch = {
        "wq": pltpu.VMEM((width, head_width), low),
        "wk": pltpu.VMEM((width, head_width), low),
        "wv": pltpu.VMEM((width, head_width), low),
        "wo": pltpu.VMEM((head_width, width), low),
        "point": pltpu.VMEM((chips, rows, width), low),
        "gain": pltpu.VMEM((1, width), full),
        "layout": pltpu.VMEM(layout.shape, jnp.int32),
        "cosine": pltpu.VMEM((length, HEAD_DIM), full),
        "sine": pltpu.VMEM((length, HEAD_DIM), full),
        "bias": pltpu.VMEM((blocks, length), full),
        "scaled": pltpu.VMEM((chips, rows, width), full),
        "pieces": pltpu.VMEM((1 + ITERS, tokens, width), low),
        "acc": pltpu.VMEM((4, tokens, head_width), full),
        "heads_out": pltpu.VMEM((3 + ITERS, seq_count, tokens, HEAD_DIM), low),
        "heads_in": pltpu.VMEM((3 + ITERS, length, HEAD_DIM), low),
        "probs": pltpu.VMEM((length, length), low),
        "key_acc": pltpu.VMEM((length, HEAD_DIM), full),
        "probs_turned": pltpu.VMEM((length, length), low),
        "grads_out": pltpu.VMEM((3 * ITERS, length, HEAD_DIM), low),
        "grads_in": pltpu.VMEM((3 * ITERS, tokens, head_width), low),
        "total": pltpu.VMEM((tokens, width), full),
        "hand_out": pltpu.VMEM((ITERS * chips, rows, width), low),
        "hand_in": pltpu.VMEM((ITERS * chips, rows, width), low),
        "far_out": pltpu.VMEM((ITERS * chips, rows, width), low),
        "far_in": pltpu.VMEM((ITERS * chips, rows, width), low),
        "normed_grad": pltpu.VMEM((rows, width), full),
        "gain_sum": pltpu.VMEM((1, width), full),
        "gain_own": pltpu.VMEM((gain_rows, HEAD_DIM), full),
        "gain_near": pltpu.VMEM((tensor_count, gain_rows, HEAD_DIM), full),
        "gain_mid": pltpu.VMEM((gain_rows, HEAD_DIM), full),
        "gain_far": pltpu.VMEM((seq_count, gain_rows, HEAD_DIM), full),
        "load_sem": dma((6,)),
        "weight_sem": dma((CHUNKS + 1,)),
        "gather_send": dma((1 + ITERS,)),
        "gather_far": dma((1 + ITERS, CHUNKS * (chips - 1))),
        "gather_near": dma((1 + ITERS, CHUNKS)),
        "heads_send": dma((3 + ITERS,)),
        "heads_recv": dma((3 + ITERS,)),
        "grads_send": dma((3 * ITERS,)),
        "grads_recv": dma((3 * ITERS,)),
        "hand_send": dma((ITERS,)),
        "hand_recv": dma((ITERS, CHUNKS)),
        "far_send": dma((ITERS,)),
        "far_recv": dma((ITERS, CHUNKS)),
        "point_send": dma((1,)),
        "point_recv": dma((1,)),
        "near_send": dma((1,)),
        "near_recv": dma((1,)),
        "wide_send": dma((1,)),
        "wide_recv": dma((1,)),
    }

    def kernel(*refs):
        point_hbm, incoming_hbm, gain_hbm, wq_hbm, wk_hbm, wv_hbm, wo_hbm = refs[:7]
        layout_hbm, cosine_hbm, sine_hbm, adjoint_out, gain_out = refs[7:12]
        r = types.SimpleNamespace(**dict(zip(scratch, refs[12:])))
        me_seq = lax.axis_index("seq")
        me = lax.axis_index("tensor")
        core = lax.rem(me, 2)
        chip = lax.div(me, 2)
        partner = me + 1 - 2 * core
        own_rows = window(me, rows)
        own_tokens = window(me_seq, tokens)
        own_columns = window(me_seq, HEAD_DIM)

        barrier = pltpu.get_barrier_semaphore()
        for step in range(1, tensor_count):
            pl.semaphore_signal(
                barrier,
                inc=1,
                device_id={"tensor": lax.rem(me + step, tensor_count)},
                device_id_type=MESH,
            )
        for mask in order:
            pl.semaphore_signal(
                barrier,
                inc=1,
                device_id={"seq": flipped(me_seq, mask, bits)},
                device_id_type=MESH,
            )

        def load(index, source, target):
            return pltpu.make_async_copy(source, target, r.load_sem.at[index])

        loads = [
            load(0, point_hbm, r.point.at[0]),
            load(1, gain_hbm, r.gain),
            load(2, incoming_hbm, r.pieces.at[1, own_rows, :]),
            load(3, layout_hbm, r.layout),
            load(4, cosine_hbm, r.cosine),
            load(5, sine_hbm, r.sine),
        ]
        for index in (0, 1, 2, 3):
            loads[index].start()

        def weight_load(item, chunk):
            source = (wq_hbm, wk_hbm, wv_hbm)[item]
            target = (r.wq, r.wk, r.wv)[item]
            place = window(chunk, part)
            return pltpu.make_async_copy(
                source.at[place, :], target.at[place, :], r.weight_sem.at[chunk]
            )

        def weight_ready(chunk):
            whole = pl.ds(0, 3 * part)
            pltpu.make_async_copy(
                wq_hbm.at[whole, :], r.wq.at[whole, :], r.weight_sem.at[chunk]
            ).wait()

        out_load = pltpu.make_async_copy(wo_hbm, r.wo, r.weight_sem.at[CHUNKS])

        def remote(source, target, send, recv, axis, peer):
            return pltpu.make_async_remote_copy(
                src_ref=source,
                dst_ref=target,
                send_sem=send,
                recv_sem=recv,
                device_id={axis: peer},
                device_id_type=MESH,
            )

        def gather_copy(item, chunk, recv, origin, peer):
            block = r.pieces.at[item, window(origin, rows), window(chunk, part)]
            return remote(block, block, r.gather_send.at[item], recv, "tensor", peer)

        def gather_far(item, chunk, step):
            peer = 2 * lax.rem(chip + step, chips) + core
            recv = r.gather_far.at[item, chunk * (chips - 1) + step - 1]
            return gather_copy(item, chunk, recv, me, peer)

        def gather_near(item, chunk):
            return gather_copy(item, chunk, r.gather_near.at[item, chunk], me, partner)

        def gather_pass(item, chunk, step):
            origin = 2 * lax.rem(chip + chips - step, chips) + core
            return gather_copy(item, chunk, r.gather_near.at[item, chunk], origin, partner)

        def gather_start(item):
            for chunk in range(CHUNKS):
                for step in range(1, chips):
                    gather_far(item, chunk, step).start()
                gather_near(item, chunk).start()

        def gather_relay(item, chunk):
            for step in range(1, chips):
                gather_far(item, chunk, step).wait_recv()
                gather_pass(item, chunk, step).start()

        def gather_ready(item, chunk):
            block = r.pieces.at[item, pl.ds(0, chips * rows), window(chunk, part)]
            send, recv = r.gather_send.at[item], r.gather_near.at[item, chunk]
            remote(block, block, send, recv, "tensor", partner).wait_recv()

        def gather_drain(item):
            block = r.pieces.at[item, pl.ds(0, (2 * chips - 1) * rows), :]
            send, recv = r.gather_send.at[item], r.gather_near.at[item, 0]
            remote(block, block, send, recv, "tensor", partner).wait_send()

        def gather_each(item, use, after=None):
            gather_relay(item, 0)

            def body(chunk, carry):
                @pl.when(chunk + 1 < CHUNKS)
                def _():
                    gather_relay(item, chunk + 1)

                if after is not None:

                    @pl.when(chunk + 2 == CHUNKS)
                    def _():
                        after()

                gather_ready(item, chunk)
                use(chunk)
                return carry

            lax.fori_loop(0, CHUNKS, body, 0)

        def point_copy(step):
            return remote(
                r.point.at[0],
                r.point.at[chips - step],
                r.point_send.at[0],
                r.point_recv.at[0],
                "tensor",
                2 * lax.rem(chip + step, chips) + core,
            )

        def heads_copy(item, mask):
            return remote(
                r.heads_out.at[item, mask],
                r.heads_in.at[item, own_tokens, :],
                r.heads_send.at[item],
                r.heads_recv.at[item],
                "seq",
                flipped(me_seq, mask, bits),
            )

        def heads_start(item, slot, turn):
            for mask in order + [0]:
                columns = window(flipped(me_seq, mask, bits), HEAD_DIM)
                values = r.acc[slot, :, columns]
                if turn:
                    values = (
                        values * r.cosine[own_tokens, :]
                        + pltpu.roll(values, HEAD_DIM // 2, 1) * r.sine[own_tokens, :]
                    )
                if mask:
                    r.heads_out[item, mask] = values.astype(low)
                else:
                    r.heads_in[item, own_tokens, :] = values.astype(low)
            for mask in order:
                heads_copy(item, mask).start()

        def heads_ready(item):
            block = r.heads_in.at[item, pl.ds(0, (seq_count - 1) * tokens), :]
            send, recv = r.heads_send.at[item], r.heads_recv.at[item]
            remote(block, block, send, recv, "seq", flipped(me_seq, 1, bits)).wait_recv()

        def heads_drain(item):
            block = r.heads_out.at[item, pl.ds(1, seq_count - 1)]
            send, recv = r.heads_send.at[item], r.heads_recv.at[item]
            remote(block, block, send, recv, "seq", flipped(me_seq, 1, bits)).wait_send()

        def grads_copy(item, mask):
            peer = flipped(me_seq, mask, bits)
            return remote(
                r.grads_out.at[item, window(peer, tokens), :],
                r.grads_in.at[item, :, own_columns],
                r.grads_send.at[item],
                r.grads_recv.at[item],
                "seq",
                peer,
            )

        def grads_start(item):
            for mask in order:
                grads_copy(item, mask).start()
            r.grads_in[item, :, own_columns] = r.grads_out[item, own_tokens, :]

        def grads_ready(item):
            block = r.grads_in.at[item, :, pl.ds(0, (seq_count - 1) * HEAD_DIM)]
            send, recv = r.grads_send.at[item], r.grads_recv.at[item]
            remote(block, block, send, recv, "seq", flipped(me_seq, 1, bits)).wait_recv()

        def grads_drain(item):
            block = r.grads_out.at[item, pl.ds(0, (seq_count - 1) * tokens), :]
            send, recv = r.grads_send.at[item], r.grads_recv.at[item]
            remote(block, block, send, recv, "seq", flipped(me_seq, 1, bits)).wait_send()

        def hand_copy(term, step, chunk):
            place = window(chunk, part)
            item = term * chips + step
            return remote(
                r.hand_out.at[item, :, place],
                r.hand_in.at[item, :, place],
                r.hand_send.at[term],
                r.hand_recv.at[term, chunk],
                "tensor",
                partner,
            )

        def far_copy(term, step, chunk):
            place = window(chunk, part)
            item = term * chips + step
            return remote(
                r.far_out.at[item, :, place],
                r.far_in.at[item, :, place],
                r.far_send.at[term],
                r.far_recv.at[term, chunk],
                "tensor",
                2 * lax.rem(chip + step, chips) + core,
            )

        def hand_ready(term, chunk):
            block = r.hand_in.at[pl.ds(term * chips, chips), :, window(chunk, part)]
            send, recv = r.hand_send.at[term], r.hand_recv.at[term, chunk]
            remote(block, block, send, recv, "tensor", partner).wait_recv()

        def far_ready(term, chunk):
            block = r.far_in.at[pl.ds(term * chips + 1, chips - 1), :, window(chunk, part)]
            send, recv = r.far_send.at[term], r.far_recv.at[term, chunk]
            remote(block, block, send, recv, "tensor", partner).wait_recv()

        def reduce_drain(term):
            block = r.hand_out.at[pl.ds(term * chips, chips)]
            send, recv = r.hand_send.at[term], r.hand_recv.at[term, 0]
            remote(block, block, send, recv, "tensor", partner).wait_send()
            block = r.far_out.at[pl.ds(term * chips + 1, chips - 1)]
            send, recv = r.far_send.at[term], r.far_recv.at[term, 0]
            remote(block, block, send, recv, "tensor", partner).wait_send()

        def wide_copy(mask, chunk):
            place = window(chunk, gain_part)
            return remote(
                r.gain_own.at[place, :],
                r.gain_far.at[mask, place, :],
                r.wide_send.at[0],
                r.wide_recv.at[0],
                "seq",
                flipped(me_seq, mask, bits),
            )

        def near_copy(step):
            return remote(
                r.gain_mid,
                r.gain_near.at[step],
                r.near_send.at[0],
                r.near_recv.at[0],
                "tensor",
                lax.rem(me + step, tensor_count),
            )

        for copy in loads[:3]:
            copy.wait()
        for chunk in range(CHUNKS):
            for item in range(3):
                weight_load(item, chunk).start()
        out_load.start()
        for copy in loads[4:]:
            copy.start()

        def scale(step):
            point = r.point[step].astype(full)
            inv_rms = lax.rsqrt(jnp.mean(point * point, axis=1, keepdims=True) + EPS)
            r.scaled[step] = point * inv_rms
            return inv_rms

        inv_rms = scale(0)
        r.pieces[0, own_rows, :] = (r.gain[...] * r.scaled[0]).astype(low)
        pl.semaphore_wait(barrier, tensor_count - 1 + seq_count - 1)
        gather_start(0)

        loads[3].wait()
        spread = (
            lax.broadcasted_iota(jnp.int32, (blocks, length), 1) // BLK
            == lax.broadcasted_iota(jnp.int32, (blocks, length), 0)
        )
        chosen = product(
            jnp.where(r.layout[...] > 0, 1.0, 0.0).astype(low),
            jnp.where(spread, 1.0, 0.0).astype(low),
            1,
            0,
        )
        earlier = (
            lax.broadcasted_iota(jnp.int32, (blocks, length), 1) // BLK
            < lax.broadcasted_iota(jnp.int32, (blocks, length), 0)
        )
        r.bias[...] = jnp.where(earlier & (chosen > 0.5), 0.0, MASKED)
        r.acc[...] = jnp.zeros(r.acc.shape, full)

        def project(chunk):
            place = window(chunk, part)
            weight_ready(chunk)
            for item, weight in enumerate((r.wq, r.wk, r.wv)):
                r.acc[item] += product(r.pieces[0, :, place], weight[place, :], 1, 0)

        gather_each(0, project, lambda: gather_start(1))
        loads[4].wait()
        loads[5].wait()
        heads_start(0, 0, True)
        heads_start(1, 1, True)
        heads_start(2, 2, False)

        def pull(item):
            def use(chunk):
                place = window(chunk, part)
                r.acc[3] += product(r.pieces[item, :, place], r.wo[:, place], 1, 1)

            return use

        out_load.wait()
        gather_each(1, pull(1))
        heads_start(3, 3, False)
        for step in range(1, chips):
            point_copy(step).start()

        block = r.point.at[pl.ds(1, chips - 1)]
        remote(block, block, r.point_send.at[0], r.point_recv.at[0], "tensor", partner).wait()
        for step in range(1, chips):
            scale(step)

        group = 2 if seq_count % 2 == 0 else 1
        heads_ready(0)
        heads_ready(1)
        sub = tokens // BLK

        def forward(base):
            span = (base + group) * tokens

            def body(step, carry):
                place = window(base + step, tokens)
                scores = product(r.heads_in[0, place, :], r.heads_in[1, :span, :], 1, 1) * score_scale
                query_at = (base + step) * tokens + lax.broadcasted_iota(jnp.int32, (tokens, span), 0)
                key_at = lax.broadcasted_iota(jnp.int32, (tokens, span), 1)
                same = (query_at // BLK == key_at // BLK) & (key_at <= query_at)
                bias = jnp.concatenate(
                    [
                        jnp.broadcast_to(r.bias[pl.ds((base + step) * sub + line, 1), :span], (BLK, span))
                        for line in range(sub)
                    ],
                    axis=0,
                )
                scores = scores + jnp.where(same, 0.0, bias)
                top = jnp.max(scores, axis=1, keepdims=True)
                weight = jnp.exp(scores - top)
                weight = weight / jnp.sum(weight, axis=1, keepdims=True)
                r.probs[place, :span] = weight.astype(low)
                r.probs_turned[:span, place] = weight.T.astype(low)
                return carry

            lax.fori_loop(0, group, body, 0)

        for base in range(0, seq_count, group):
            forward(base)

        def turned_back(values, place):
            return (
                values * r.cosine[place, :]
                - pltpu.roll(values, HEAD_DIM // 2, 1) * r.sine[place, :]
            ).astype(low)

        def backward(term):
            r.key_acc[...] = jnp.zeros(r.key_acc.shape, full)
            for base in range(0, seq_count, group):
                later = slice(base * tokens, length)
                for step in range(group):
                    place = slice((base + step) * tokens, (base + step + 1) * tokens)
                    r.grads_out[3 * term + 2, place, :] = product(
                        r.probs_turned[place, later], r.heads_in[3 + term, later, :], 1, 0
                    ).astype(low)
            grads_start(3 * term + 2)

            def at(base):
                span = (base + group) * tokens

                def body(step, carry):
                    place = window(base + group - 1 - step, tokens)
                    probs = r.probs[place, :span]
                    grad_low = r.heads_in[3 + term, place, :]
                    grad_probs = product(grad_low, r.heads_in[2, :span, :], 1, 1)
                    wide = probs.astype(full)
                    delta = jnp.sum(wide * grad_probs, axis=1, keepdims=True)
                    grad_scores = (wide * (grad_probs - delta)).astype(low)
                    grad_query = product(grad_scores, r.heads_in[1, :span, :], 1, 0) * score_scale
                    r.grads_out[3 * term, place, :] = turned_back(grad_query, place)
                    r.key_acc[:span, :] += product(grad_scores, r.heads_in[0, place, :], 0, 0)
                    return carry

                lax.fori_loop(0, group, body, 0)

            for base in reversed(range(0, seq_count, group)):
                at(base)
            r.grads_out[3 * term + 1] = turned_back(r.key_acc[...] * score_scale, slice(None))
            grads_start(3 * term + 1)
            grads_start(3 * term)

        def hand_on(term, chunk):
            place = window(chunk, part)
            hand_ready(term, chunk)
            gain_term = jnp.zeros((1, part), full)
            for step in range(chips):
                owner = 2 * lax.rem(chip + step, chips) + core
                pair = r.total[window(owner, rows), place] + r.hand_in[
                    term * chips + step, :, place
                ].astype(full)
                if step:
                    r.far_out[term * chips + step, :, place] = pair.astype(low)
                    far_copy(term, step, chunk).start()
                else:
                    r.normed_grad[:, place] = pair
                gain_term += jnp.sum(pair * r.scaled[step, :, place], axis=0, keepdims=True)
            if term:
                gain_term += r.gain_sum[:, place]
            if term < ITERS - 1:
                r.gain_sum[:, place] = gain_term
                return
            r.gain_own[window(chunk, gain_part), :] = jnp.concatenate(
                [gain_term[:, line * HEAD_DIM : (line + 1) * HEAD_DIM] for line in range(gain_part)],
                axis=0,
            )
            for mask in order:
                wide_copy(mask, chunk).start()

        def push(term):
            for item, weight in ((2, r.wv), (1, r.wk)):
                grads_ready(3 * term + item)

                def body(chunk, carry):
                    place = window(chunk, part)
                    value = product(r.grads_in[3 * term + item], weight[place, :], 1, 1)
                    if item == 1:
                        value = value + r.total[:, place]
                    r.total[:, place] = value
                    return carry

                lax.fori_loop(0, CHUNKS, body, 0)
            grads_ready(3 * term)

            def last(chunk, carry):
                place = window(chunk, part)
                r.total[:, place] += product(r.grads_in[3 * term], r.wq[place, :], 1, 1)
                for step in range(chips):
                    other = 2 * lax.rem(chip + step, chips) + 1 - core
                    r.hand_out[term * chips + step, :, place] = r.total[
                        window(other, rows), place
                    ].astype(low)
                for step in range(chips):
                    hand_copy(term, step, chunk).start()

                @pl.when(chunk > 0)
                def _():
                    hand_on(term, chunk - 1)

                return carry

            lax.fori_loop(0, CHUNKS, last, 0)
            hand_on(term, CHUNKS - 1)

        for term in range(ITERS):
            if term:
                r.acc[3] = jnp.zeros((tokens, head_width), full)
                gather_start(1 + term)
                gather_each(1 + term, pull(1 + term))
                heads_start(3 + term, 3, False)
            else:
                heads_ready(2)
            heads_ready(3 + term)
            backward(term)
            push(term)
            final = term == ITERS - 1
            for chunk in range(CHUNKS):
                place = slice(chunk * part, (chunk + 1) * part)
                value = r.normed_grad[:, place]
                far_ready(term, chunk)
                for step in range(1, chips):
                    value = value + r.far_in[term * chips + step, :, place].astype(full)
                r.normed_grad[:, place] = value
            weighted = r.gain[...] * r.normed_grad[...]
            inner = jnp.sum(weighted * r.scaled[0], axis=1, keepdims=True)
            cotangent = inv_rms * (weighted - r.scaled[0] * (inner / width))
            if term == 0:
                adjoint_out[...] = cotangent
            else:
                adjoint_out[...] += cotangent
            if not final:
                r.pieces[2 + term, own_rows, :] = cotangent.astype(low)

        for item in range(1 + ITERS):
            gather_drain(item)
        for item in range(3 + ITERS):
            heads_drain(item)
        for item in range(3 * ITERS):
            grads_drain(item)
        for term in range(ITERS):
            reduce_drain(term)
        block = r.gain_far.at[pl.ds(1, seq_count - 1)]
        remote(
            block, block, r.wide_send.at[0], r.wide_recv.at[0], "seq", flipped(me_seq, 1, bits)
        ).wait()
        value = r.gain_own[...]
        for mask in order:
            value = value + r.gain_far[mask]
        r.gain_mid[...] = value
        for step in range(1, tensor_count):
            near_copy(step).start()
        block = r.gain_near.at[pl.ds(1, tensor_count - 1)]
        remote(block, block, r.near_send.at[0], r.near_recv.at[0], "tensor", partner).wait()
        for step in range(1, tensor_count):
            value = value + r.gain_near[step]
        gain_out[...] = value

    anywhere = pl.BlockSpec(memory_space=pl.ANY)
    adjoint, gain_grad = pl.pallas_call(
        kernel,
        out_shape=[
            jax.ShapeDtypeStruct((rows, width), full),
            jax.ShapeDtypeStruct((gain_rows, HEAD_DIM), full),
        ],
        in_specs=[anywhere] * 10,
        out_specs=[pl.BlockSpec(memory_space=pltpu.VMEM)] * 2,
        scratch_shapes=list(scratch.values()),
        compiler_params=pltpu.CompilerParams(
            collective_id=0, has_side_effects=True, vmem_limit_bytes=62 << 20
        ),
    )(
        fixed_point,
        incoming,
        norm_gain.reshape(1, width),
        query_weight,
        key_weight,
        value_weight,
        out_weight,
        layout,
        jnp.asarray(cosine),
        jnp.asarray(sine),
    )
    adjoint = incoming.astype(full) + adjoint
    return adjoint, gain_grad.reshape(width) * length ** (-0.5)


def solution(mesh):
    in_specs = (
        P(("seq", "tensor"), None),
        P(("seq", "tensor"), None),
        P(),
        P(None, "tensor"),
        P(None, "tensor"),
        P(None, "tensor"),
        P("tensor", None),
        P(),
    )
    out_specs = (P(("seq", "tensor"), None), P())
    seq, tensor = mesh.shape["seq"], mesh.shape["tensor"]

    def body(*arrays):
        heads = arrays[3].shape[1] * tensor // HEAD_DIM
        tokens = arrays[0].shape[0] * tensor
        fits = (
            tensor % 2 == 0
            and seq & (seq - 1) == 0
            and heads == seq * tensor
            and tokens % 128 == 0
            and arrays[0].shape[0] % 16 == 0
            and arrays[0].shape[1] % (8 * HEAD_DIM * CHUNKS) == 0
        )
        return (fused_body if fits else ring_body)(*arrays)

    return jax.shard_map(body, mesh=mesh, in_specs=in_specs, out_specs=out_specs, check_vma=False)
```

```python
import types

import jax
import jax.numpy as jnp
import numpy as np
from jax import lax
from jax.experimental import pallas as pl
from jax.experimental.pallas import tpu as pltpu
from jax.sharding import PartitionSpec as P

HEAD_DIM = 128
BLK = 64
ITERS = 2


EPS = 1e-05
THETA = 10000.0
MASKED = -1e30


def rope_tables(positions):
    freq = THETA ** (-jnp.arange(0, HEAD_DIM, 2, dtype=jnp.float32) / HEAD_DIM)
    angle = positions.astype(jnp.float32)[:, None] * freq[None, :]
    cosine = jnp.concatenate([jnp.cos(angle), jnp.cos(angle)], axis=1)[:, None, :]
    sine = jnp.concatenate([jnp.sin(angle), jnp.sin(angle)], axis=1)[:, None, :]
    return (cosine, sine)


def rotate(values, cosine, sine):
    half = HEAD_DIM // 2
    turned = jnp.concatenate([-values[..., half:], values[..., :half]], axis=-1)
    return values * cosine + turned * sine


def rotate_back(values, cosine, sine):
    half = HEAD_DIM // 2
    weighted = values * sine
    turned = jnp.concatenate([weighted[..., half:], -weighted[..., :half]], axis=-1)
    return values * cosine + turned


def expand_blocks(chosen):
    return jnp.repeat(jnp.repeat(chosen, BLK, axis=0), BLK, axis=1)


def pair_mask(query_pos, key_pos, chosen):
    query_block = (query_pos // BLK)[:, None]
    key_block = (key_pos // BLK)[None, :]
    earlier = (key_block < query_block) & chosen
    same = (key_block == query_block) & (key_pos[None, :] <= query_pos[:, None])
    return earlier | same


def ring_body(
    fixed_point, incoming, norm_gain, query_weight, key_weight, value_weight, out_weight, layout
):
    local_rows, model_width = fixed_point.shape
    head_width = query_weight.shape[1]
    head_count = head_width // HEAD_DIM
    seq_tokens = local_rows * lax.axis_size("tensor")
    seq_length = seq_tokens * lax.axis_size("seq")
    seq_index = lax.axis_index("seq")
    score_scale = HEAD_DIM ** (-0.5)
    contract_last = (((1,), (1,)), ((), ()))
    head_shape = (seq_tokens, head_count, HEAD_DIM)
    point = fixed_point.astype(jnp.float32)
    inv_rms = lax.rsqrt(jnp.mean(point * point, axis=1, keepdims=True) + EPS)
    scaled = point * inv_rms
    normed = (norm_gain * scaled).astype(jnp.bfloat16)
    project_piece = lax.all_gather(normed, "tensor", axis=0, tiled=True)
    projected = jnp.concatenate(
        [
            jnp.dot(project_piece, query_weight, preferred_element_type=jnp.float32),
            jnp.dot(project_piece, key_weight, preferred_element_type=jnp.float32),
            jnp.dot(project_piece, value_weight, preferred_element_type=jnp.float32),
        ],
        axis=1,
    )
    positions = seq_index * seq_tokens + jnp.arange(seq_tokens, dtype=jnp.int32)
    cosine, sine = rope_tables(positions)
    queries = rotate(projected[:, :head_width].reshape(head_shape), cosine, sine).astype(
        jnp.bfloat16
    )
    keys = rotate(
        projected[:, head_width : 2 * head_width].reshape(head_shape), cosine, sine
    ).astype(jnp.bfloat16)
    values = projected[:, 2 * head_width :].reshape(head_shape).astype(jnp.bfloat16)
    block_rows = seq_tokens // BLK
    block_count = seq_length // BLK
    first_block = seq_index * block_rows
    key_positions = jnp.arange(seq_length, dtype=jnp.int32)
    chosen_rows = (
        lax.dynamic_slice(layout, (first_block, jnp.int32(0)), (block_rows, block_count)) > 0
    )
    allowed = pair_mask(positions, key_positions, expand_blocks(chosen_rows))
    keys_all, values_all = (
        lax.all_gather(keys, "seq", axis=0, tiled=True),
        lax.all_gather(values, "seq", axis=0, tiled=True),
    )
    scores = (
        jnp.einsum("qhd,khd->hqk", queries, keys_all, preferred_element_type=jnp.float32)
        * score_scale
    )
    scores = jnp.where(allowed[None], scores, MASKED)
    log_norm = jax.nn.logsumexp(scores, axis=2, keepdims=True)
    probs = jnp.exp(scores - log_norm)
    probs_low = probs.astype(jnp.bfloat16)
    attended = jnp.einsum(
        "hqk,khd->qhd", probs_low, values_all, preferred_element_type=jnp.float32
    ).astype(jnp.bfloat16)
    cotangent = incoming.astype(jnp.float32)
    adjoint = cotangent
    gain_grad = jnp.zeros((model_width,), jnp.float32)
    for term_index in range(ITERS):
        grad_out = lax.dot_general(
            lax.all_gather(cotangent.astype(jnp.bfloat16), "tensor", axis=0, tiled=True),
            out_weight,
            contract_last,
            preferred_element_type=jnp.float32,
        )
        grad_low = grad_out.astype(jnp.bfloat16).reshape(head_shape)
        delta = jnp.sum(grad_low.astype(jnp.float32) * attended.astype(jnp.float32), axis=2)
        grad_probs = jnp.einsum(
            "qhd,khd->hqk", grad_low, values_all, preferred_element_type=jnp.float32
        )
        grad_scores = (probs * (grad_probs - delta.T[:, :, None])).astype(jnp.bfloat16)
        grad_query = (
            jnp.einsum("hqk,khd->qhd", grad_scores, keys_all, preferred_element_type=jnp.float32)
            * score_scale
        )
        key_part = (
            jnp.einsum("hqk,qhd->khd", grad_scores, queries, preferred_element_type=jnp.float32)
            * score_scale
        )
        value_part = jnp.einsum(
            "hqk,qhd->khd", probs_low, grad_low, preferred_element_type=jnp.float32
        )
        key_grads = lax.psum_scatter(
            jnp.concatenate(
                [
                    key_part.reshape(seq_tokens * lax.axis_size("seq"), head_width),
                    value_part.reshape(seq_tokens * lax.axis_size("seq"), head_width),
                ],
                axis=1,
            ).astype(jnp.bfloat16),
            "seq",
            scatter_dimension=0,
            tiled=True,
        ).astype(jnp.float32)
        grad_key = key_grads[:, :head_width].reshape(head_shape)
        grad_value = key_grads[:, head_width:].reshape(head_shape)
        query_low = (
            rotate_back(grad_query, cosine, sine)
            .astype(jnp.bfloat16)
            .reshape(seq_tokens, head_width)
        )
        key_low = (
            rotate_back(grad_key, cosine, sine).astype(jnp.bfloat16).reshape(seq_tokens, head_width)
        )
        value_low = grad_value.astype(jnp.bfloat16).reshape(seq_tokens, head_width)
        total = lax.dot_general(
            query_low, query_weight, contract_last, preferred_element_type=jnp.float32
        )
        total = total + lax.dot_general(
            key_low, key_weight, contract_last, preferred_element_type=jnp.float32
        )
        total = total + lax.dot_general(
            value_low, value_weight, contract_last, preferred_element_type=jnp.float32
        )
        grad_normed = lax.psum_scatter(
            total.astype(jnp.bfloat16), "tensor", scatter_dimension=0, tiled=True
        ).astype(jnp.float32)
        gain_term = jnp.sum(grad_normed * scaled, axis=0)
        gain_grad = gain_grad + lax.psum(gain_term, ("seq", "tensor"))
        weighted = norm_gain * grad_normed
        inner = jnp.sum(weighted * scaled, axis=1, keepdims=True)
        cotangent = inv_rms * (weighted - scaled * (inner / model_width))
        adjoint = adjoint + cotangent
    return (adjoint, gain_grad * seq_length ** (-0.5))


CHUNKS = 4
HALVES = 2
MESH = pl.DeviceIdType.MESH


def numpy_tables(length):
    freq = np.float32(THETA) ** (-np.arange(0, HEAD_DIM, 2, dtype=np.float32) / np.float32(HEAD_DIM))
    angle = np.arange(length, dtype=np.float32)[:, None] * freq.astype(np.float32)[None, :]
    cosine = np.cos(angle.astype(np.float64)).astype(np.float32)
    sine = np.sin(angle.astype(np.float64)).astype(np.float32)
    return np.concatenate([cosine, cosine], axis=1), np.concatenate([-sine, sine], axis=1)


def product(left, right, left_dim, right_dim):
    return lax.dot_general(
        left, right, (((left_dim,), (right_dim,)), ((), ())), preferred_element_type=jnp.float32
    )


def flipped(index, mask, bits):
    result = 0
    for bit in range(bits):
        here = lax.rem(lax.div(index, 1 << bit), 2)
        result = result + (1 << bit) * ((1 - here) if (mask >> bit) & 1 else here)
    return result


def window(index, size):
    return pl.ds(pl.multiple_of(index * size, size), size)


def fused_body(
    fixed_point, incoming, norm_gain, query_weight, key_weight, value_weight, out_weight, layout
):
    rows, width = fixed_point.shape
    tensor_count = lax.axis_size("tensor")
    seq_count = lax.axis_size("seq")
    chips = tensor_count // 2
    bits = seq_count.bit_length() - 1
    head_width = query_weight.shape[1]
    tokens = rows * tensor_count
    length = tokens * seq_count
    blocks = layout.shape[0]
    part = width // CHUNKS
    lines = rows // HALVES
    groups = length // rows
    half_tokens = tensor_count * lines
    score_scale = HEAD_DIM ** (-0.5)
    gain_rows = width // HEAD_DIM
    gain_part = gain_rows // CHUNKS
    cosine, sine = numpy_tables(length)
    order = list(range(seq_count - 1, 0, -1))
    low, full = jnp.bfloat16, jnp.float32
    dma = pltpu.SemaphoreType.DMA
    scratch = {
        "weights": pltpu.VMEM((4 * CHUNKS + 1, part, head_width), low),
        "point": pltpu.VMEM((chips, HALVES, lines, width), low),
        "gain": pltpu.VMEM((1, width), full),
        "layout": pltpu.VMEM(layout.shape, jnp.int32),
        "cosine": pltpu.VMEM((length, HEAD_DIM), full),
        "sine": pltpu.VMEM((length, HEAD_DIM), full),
        "bias": pltpu.VMEM((blocks, length), full),
        "scaled": pltpu.VMEM((chips, HALVES, lines, width), full),
        "pieces": pltpu.VMEM((2, tokens, width), low),
        "series": pltpu.VMEM((ITERS - 1, HALVES, tensor_count, lines, width), low),
        "heads_out": pltpu.VMEM((4, seq_count, tokens, HEAD_DIM), low),
        "heads_in": pltpu.VMEM((4, length, HEAD_DIM), low),
        "late_out": pltpu.VMEM(
            (ITERS - 1, HALVES, seq_count, tensor_count, lines, HEAD_DIM), low
        ),
        "late_in": pltpu.VMEM((ITERS - 1, groups, HALVES, lines, HEAD_DIM), low),
        "probs": pltpu.VMEM((length, length), low),
        "key_acc": pltpu.VMEM((length, HEAD_DIM), full),
        "probs_turned": pltpu.VMEM((length, length), low),
        "grads_out": pltpu.VMEM((2 * ITERS, length, HEAD_DIM), low),
        "grads_in": pltpu.VMEM((2 * ITERS, tokens, head_width), low),
        "query_out": pltpu.VMEM((ITERS, groups, HALVES, lines, HEAD_DIM), low),
        "query_in": pltpu.VMEM((ITERS, HALVES, tensor_count, lines, head_width), low),
        "total": pltpu.VMEM((tensor_count, HALVES, lines, width), full),
        "hand_out": pltpu.VMEM((ITERS, HALVES, chips, lines, width), low),
        "hand_in": pltpu.VMEM((ITERS, HALVES, chips, lines, width), low),
        "far_out": pltpu.VMEM((ITERS, HALVES, chips - 1, lines, width), low),
        "far_in": pltpu.VMEM((ITERS, HALVES, chips - 1, lines, width), low),
        "normed_grad": pltpu.VMEM((HALVES, lines, width), full),
        "gain_sum": pltpu.VMEM((1, width), full),
        "gain_own": pltpu.VMEM((gain_rows, HEAD_DIM), full),
        "gain_near": pltpu.VMEM((tensor_count, gain_rows, HEAD_DIM), full),
        "gain_mid": pltpu.VMEM((gain_rows, HEAD_DIM), full),
        "gain_far": pltpu.VMEM((seq_count, gain_rows, HEAD_DIM), full),
        "load_sem": dma((6,)),
        "weight_sem": dma((CHUNKS + 1,)),
        "gather_send": dma((2,)),
        "gather_far": dma((2, CHUNKS * (chips - 1))),
        "gather_near": dma((2, CHUNKS)),
        "series_send": dma(((ITERS - 1) * HALVES,)),
        "series_far": dma(((ITERS - 1) * HALVES, CHUNKS * (chips - 1))),
        "series_near": dma(((ITERS - 1) * HALVES, CHUNKS)),
        "heads_send": dma((4,)),
        "heads_recv": dma((4,)),
        "late_send": dma(((ITERS - 1) * HALVES,)),
        "late_recv": dma(((ITERS - 1) * HALVES,)),
        "grads_send": dma((2 * ITERS,)),
        "grads_recv": dma((2 * ITERS,)),
        "query_send": dma((ITERS * HALVES,)),
        "query_recv": dma((ITERS * HALVES,)),
        "hand_send": dma((ITERS,)),
        "hand_recv": dma((ITERS * HALVES, CHUNKS)),
        "far_send": dma((ITERS,)),
        "far_recv": dma((ITERS * HALVES, CHUNKS)),
        "point_send": dma((1,)),
        "point_recv": dma((1,)),
        "near_send": dma((1,)),
        "near_recv": dma((1,)),
        "wide_send": dma((1,)),
        "wide_recv": dma((1,)),
    }

    def kernel(*refs):
        point_hbm, incoming_hbm, gain_hbm, wq_hbm, wk_hbm, wv_hbm, wo_hbm = refs[:7]
        layout_hbm, cosine_hbm, sine_hbm, adjoint_out, gain_out = refs[7:12]
        r = types.SimpleNamespace(**dict(zip(scratch, refs[12:])))
        me_seq = lax.axis_index("seq")
        me = lax.axis_index("tensor")
        core = lax.rem(me, 2)
        chip = lax.div(me, 2)
        partner = me + 1 - 2 * core
        own_rows = window(me, rows)
        own_tokens = window(me_seq, tokens)
        own_columns = window(me_seq, HEAD_DIM)

        barrier = pltpu.get_barrier_semaphore()
        for step in range(1, tensor_count):
            pl.semaphore_signal(
                barrier,
                inc=1,
                device_id={"tensor": lax.rem(me + step, tensor_count)},
                device_id_type=MESH,
            )
        for mask in order:
            pl.semaphore_signal(
                barrier,
                inc=1,
                device_id={"seq": flipped(me_seq, mask, bits)},
                device_id_type=MESH,
            )

        def load(index, source, target):
            return pltpu.make_async_copy(source, target, r.load_sem.at[index])

        loads = [
            load(0, point_hbm, r.point.at[0]),
            load(1, gain_hbm, r.gain),
            load(2, incoming_hbm, r.pieces.at[1, own_rows, :]),
            load(3, layout_hbm, r.layout),
            load(4, cosine_hbm, r.cosine),
            load(5, sine_hbm, r.sine),
        ]
        for index in (0, 1, 2, 3):
            loads[index].start()

        def block_of(item, chunk):
            return item * CHUNKS + chunk

        def weight_load(item, chunk):
            if item == 3:
                source = wo_hbm.at[:, window(chunk, part)]
            else:
                source = (wv_hbm, wk_hbm, wq_hbm)[item].at[chunk]
            target = r.weights.at[1 + block_of(item, chunk)]
            return pltpu.make_async_copy(
                source, target, r.weight_sem.at[CHUNKS if item == 3 else chunk]
            )

        def weight_ready(index, count):
            pltpu.make_async_copy(
                wq_hbm.at[pl.ds(0, count)], r.weights.at[pl.ds(0, count)], r.weight_sem.at[index]
            ).wait()

        def turn_weights(first, last):
            def body(block, carry):
                for line in range(0, part, HEAD_DIM):
                    strip = slice(line, line + HEAD_DIM)
                    r.weights[block, :, strip] = r.weights[block + 1, strip, :].T
                return carry

            lax.fori_loop(first * CHUNKS, last * CHUNKS, body, 0)

        def remote(source, target, send, recv, axis, peer):
            return pltpu.make_async_remote_copy(
                src_ref=source,
                dst_ref=target,
                send_sem=send,
                recv_sem=recv,
                device_id={axis: peer},
                device_id_type=MESH,
            )

        def gather_parts(item, chunk, origin):
            place = window(chunk, part)
            if isinstance(item, tuple):
                term, half = item
                index = (term - 1) * HALVES + half
                block = r.series.at[term - 1, half, origin, :, place]
                return block, r.series_send.at[index], r.series_far, r.series_near, index
            block = r.pieces.at[item, window(origin, rows), place]
            return block, r.gather_send.at[item], r.gather_far, r.gather_near, item

        def gather_far(item, chunk, step):
            block, send, far, near, index = gather_parts(item, chunk, me)
            recv = far.at[index, chunk * (chips - 1) + step - 1]
            peer = 2 * lax.rem(chip + step, chips) + core
            return remote(block, block, send, recv, "tensor", peer)

        def gather_near(item, chunk):
            block, send, far, near, index = gather_parts(item, chunk, me)
            return remote(block, block, send, near.at[index, chunk], "tensor", partner)

        def gather_pass(item, chunk, step):
            origin = 2 * lax.rem(chip + chips - step, chips) + core
            block, send, far, near, index = gather_parts(item, chunk, origin)
            return remote(block, block, send, near.at[index, chunk], "tensor", partner)

        def gather_start(item):
            for chunk in range(CHUNKS):
                for step in range(1, chips):
                    gather_far(item, chunk, step).start()
                gather_near(item, chunk).start()

        def gather_relay(item, chunk):
            for step in range(1, chips):
                gather_far(item, chunk, step).wait_recv()
                gather_pass(item, chunk, step).start()

        def gather_ready(item, chunk):
            place = window(chunk, part)
            block, send, far, near, index = gather_parts(item, chunk, 0)
            if isinstance(item, tuple):
                block = r.series.at[item[0] - 1, item[1], pl.ds(0, chips), :, place]
            else:
                block = r.pieces.at[item, pl.ds(0, chips * rows), place]
            remote(block, block, send, near.at[index, chunk], "tensor", partner).wait_recv()

        def gather_drain(item):
            block, send, far, near, index = gather_parts(item, 0, 0)
            if isinstance(item, tuple):
                block = r.series.at[item[0] - 1, item[1], pl.ds(0, 2 * chips - 1)]
            else:
                block = r.pieces.at[item, pl.ds(0, (2 * chips - 1) * rows), :]
            remote(block, block, send, near.at[index, 0], "tensor", partner).wait_send()

        def gather_each(item, use, after=None, count=CHUNKS):
            gather_relay(item, 0)

            def body(chunk, carry):
                @pl.when(chunk + 1 < CHUNKS)
                def _():
                    gather_relay(item, chunk + 1)

                if after is not None:

                    @pl.when(chunk + 2 == CHUNKS)
                    def _():
                        after()

                gather_ready(item, chunk)
                use(chunk)
                return carry

            lax.fori_loop(0, count, body, 0)

        def columns_of(slot):
            return slice(slot * head_width, (slot + 1) * head_width)

        def point_copy(step):
            return remote(
                r.point.at[0],
                r.point.at[chips - step],
                r.point_send.at[0],
                r.point_recv.at[0],
                "tensor",
                2 * lax.rem(chip + step, chips) + core,
            )

        def heads_copy(item, mask):
            return remote(
                r.heads_out.at[item, mask],
                r.heads_in.at[item, own_tokens, :],
                r.heads_send.at[item],
                r.heads_recv.at[item],
                "seq",
                flipped(me_seq, mask, bits),
            )

        def heads_start(item, turn):
            for mask in order + [0]:
                peer = flipped(me_seq, mask, bits)
                columns = window(item * seq_count + peer, HEAD_DIM)
                values = r.total[:, :, :, columns].reshape(tokens, HEAD_DIM)
                if turn:
                    values = (
                        values * r.cosine[own_tokens, :]
                        + pltpu.roll(values, HEAD_DIM // 2, 1) * r.sine[own_tokens, :]
                    )
                if mask:
                    r.heads_out[item, mask] = values.astype(low)
                else:
                    r.heads_in[item, own_tokens, :] = values.astype(low)
            for mask in order:
                heads_copy(item, mask).start()

        def late_copy(term, half, mask):
            index = (term - 1) * HALVES + half
            return remote(
                r.late_out.at[term - 1, half, mask],
                r.late_in.at[term - 1, window(me_seq, tensor_count), half],
                r.late_send.at[index],
                r.late_recv.at[index],
                "seq",
                flipped(me_seq, mask, bits),
            )

        def late_start(term, half):
            for mask in order + [0]:
                columns = window(flipped(me_seq, mask, bits), HEAD_DIM)
                values = r.total[:, half, :, columns].astype(low)
                if mask:
                    r.late_out[term - 1, half, mask] = values
                else:
                    r.late_in[term - 1, window(me_seq, tensor_count), half] = values
            for mask in order:
                late_copy(term, half, mask).start()

        def late_whole(term, half):
            block = r.late_out.at[term - 1, half, pl.ds(1, seq_count - 1)]
            index = (term - 1) * HALVES + half
            send, recv = r.late_send.at[index], r.late_recv.at[index]
            return remote(block, block, send, recv, "seq", flipped(me_seq, 1, bits))

        def heads_ready(item):
            block = r.heads_in.at[item, pl.ds(0, (seq_count - 1) * tokens), :]
            send, recv = r.heads_send.at[item], r.heads_recv.at[item]
            remote(block, block, send, recv, "seq", flipped(me_seq, 1, bits)).wait_recv()

        def heads_drain(item):
            block = r.heads_out.at[item, pl.ds(1, seq_count - 1)]
            send, recv = r.heads_send.at[item], r.heads_recv.at[item]
            remote(block, block, send, recv, "seq", flipped(me_seq, 1, bits)).wait_send()

        def grads_copy(item, mask):
            peer = flipped(me_seq, mask, bits)
            return remote(
                r.grads_out.at[item, window(peer, tokens), :],
                r.grads_in.at[item, :, own_columns],
                r.grads_send.at[item],
                r.grads_recv.at[item],
                "seq",
                peer,
            )

        def grads_start(item):
            for mask in order:
                grads_copy(item, mask).start()
            r.grads_in[item, :, own_columns] = r.grads_out[item, own_tokens, :]

        def grads_ready(item):
            block = r.grads_in.at[item, :, pl.ds(0, (seq_count - 1) * HEAD_DIM)]
            send, recv = r.grads_send.at[item], r.grads_recv.at[item]
            remote(block, block, send, recv, "seq", flipped(me_seq, 1, bits)).wait_recv()

        def grads_drain(item):
            block = r.grads_out.at[item, pl.ds(0, (seq_count - 1) * tokens), :]
            send, recv = r.grads_send.at[item], r.grads_recv.at[item]
            remote(block, block, send, recv, "seq", flipped(me_seq, 1, bits)).wait_send()

        def query_copy(term, half, mask):
            peer = flipped(me_seq, mask, bits)
            index = term * HALVES + half
            return remote(
                r.query_out.at[term, window(peer, tensor_count), half],
                r.query_in.at[term, half, :, :, own_columns],
                r.query_send.at[index],
                r.query_recv.at[index],
                "seq",
                peer,
            )

        def query_start(term):
            for half in range(HALVES):
                for mask in order:
                    query_copy(term, half, mask).start()
                own = r.query_out[term, window(me_seq, tensor_count), half]
                r.query_in[term, half, :, :, own_columns] = own

        def query_whole(term, half):
            block = r.query_in.at[term, half, :, :, pl.ds(0, (seq_count - 1) * HEAD_DIM)]
            index = term * HALVES + half
            send, recv = r.query_send.at[index], r.query_recv.at[index]
            return remote(block, block, send, recv, "seq", flipped(me_seq, 1, bits))

        def hand_copy(term, half, chunk):
            place = window(chunk, part)
            return remote(
                r.hand_out.at[term, half, :, :, place],
                r.hand_in.at[term, half, :, :, place],
                r.hand_send.at[term],
                r.hand_recv.at[term * HALVES + half, chunk],
                "tensor",
                partner,
            )

        def far_copy(term, half, step, chunk):
            place = window(chunk, part)
            return remote(
                r.far_out.at[term, half, step - 1, :, place],
                r.far_in.at[term, half, step - 1, :, place],
                r.far_send.at[term],
                r.far_recv.at[term * HALVES + half, chunk],
                "tensor",
                2 * lax.rem(chip + step, chips) + core,
            )

        def far_ready(term, half, chunk):
            block = r.far_in.at[term, half, :, :, window(chunk, part)]
            send, recv = r.far_send.at[term], r.far_recv.at[term * HALVES + half, chunk]
            remote(block, block, send, recv, "tensor", partner).wait_recv()

        def reduce_drain(term):
            block = r.hand_out.at[term]
            send, recv = r.hand_send.at[term], r.hand_recv.at[term * HALVES, 0]
            remote(block, block, send, recv, "tensor", partner).wait_send()
            block = r.far_out.at[term]
            send, recv = r.far_send.at[term], r.far_recv.at[term * HALVES, 0]
            remote(block, block, send, recv, "tensor", partner).wait_send()

        def wide_copy(mask, chunk):
            place = window(chunk, gain_part)
            return remote(
                r.gain_own.at[place, :],
                r.gain_far.at[mask, place, :],
                r.wide_send.at[0],
                r.wide_recv.at[0],
                "seq",
                flipped(me_seq, mask, bits),
            )

        def near_copy(step):
            return remote(
                r.gain_mid,
                r.gain_near.at[step],
                r.near_send.at[0],
                r.near_recv.at[0],
                "tensor",
                lax.rem(me + step, tensor_count),
            )

        for copy in loads[:3]:
            copy.wait()
        for chunk in range(CHUNKS):
            for item in range(3):
                weight_load(item, chunk).start()
        for chunk in range(CHUNKS):
            weight_load(3, chunk).start()
        for copy in loads[4:]:
            copy.start()

        def scale(step):
            point = r.point[step].astype(full)
            inv_rms = lax.rsqrt(jnp.mean(point * point, axis=-1, keepdims=True) + EPS)
            r.scaled[step] = point * inv_rms
            return inv_rms

        inv_rms = scale(0)
        normed = r.gain[...].reshape(1, 1, width) * r.scaled[0]
        r.pieces[0, own_rows, :] = normed.astype(low).reshape(rows, width)
        pl.semaphore_wait(barrier, tensor_count - 1 + seq_count - 1)
        gather_start(0)

        loads[3].wait()
        spread = (
            lax.broadcasted_iota(jnp.int32, (blocks, length), 1) // BLK
            == lax.broadcasted_iota(jnp.int32, (blocks, length), 0)
        )
        chosen = product(
            jnp.where(r.layout[...] > 0, 1.0, 0.0).astype(low),
            jnp.where(spread, 1.0, 0.0).astype(low),
            1,
            0,
        )
        earlier = (
            lax.broadcasted_iota(jnp.int32, (blocks, length), 1) // BLK
            < lax.broadcasted_iota(jnp.int32, (blocks, length), 0)
        )
        r.bias[...] = jnp.where(earlier & (chosen > 0.5), 0.0, MASKED)
        r.total[...] = jnp.zeros(r.total.shape, full)
        spread_rows = (tensor_count, HALVES, lines, head_width)

        def project_one(item, chunk):
            place = window(chunk, part)
            weight = r.weights[1 + block_of(2 - item, chunk)]
            value = product(r.pieces[0, :, place], weight, 1, 0)
            r.total[:, :, :, columns_of(item)] += value.reshape(spread_rows)

        def project(chunk):
            weight_ready(chunk, 3)
            for item in range(3):
                project_one(item, chunk)

        gather_each(0, project, lambda: gather_start(1), CHUNKS - 1)
        for copy in loads[4:]:
            copy.wait()
        gather_ready(0, CHUNKS - 1)
        weight_ready(CHUNKS - 1, 3)
        for item in range(3):
            project_one(item, CHUNKS - 1)
            heads_start(item, item < 2)
        weight_ready(CHUNKS, CHUNKS)

        def pull_first(chunk):
            place = window(chunk, part)
            weight = r.weights[1 + block_of(3, chunk)]
            value = product(r.pieces[1, :, place], weight, 1, 1)
            r.total[:, :, :, columns_of(3)] += value.reshape(spread_rows)

        gather_each(1, pull_first)
        heads_start(3, False)

        def pull(term, half):
            def use(chunk):
                place = window(chunk, part)
                piece = r.series[term - 1, half, :, :, place].reshape(half_tokens, part)
                value = product(piece, r.weights[block_of(3, chunk)], 1, 0)
                r.total[:, half, :, :head_width] += value.reshape(tensor_count, lines, head_width)

            return use
        for step in range(1, chips):
            point_copy(step).start()
        turn_weights(0, 3)

        block = r.point.at[pl.ds(1, chips - 1)]
        remote(block, block, r.point_send.at[0], r.point_recv.at[0], "tensor", partner).wait()
        for step in range(1, chips):
            scale(step)

        group = 2 if seq_count % 2 == 0 else 1
        heads_ready(0)
        heads_ready(1)
        sub = tokens // BLK

        def forward(base):
            span = (base + group) * tokens

            def body(step, carry):
                place = window(base + step, tokens)
                scores = product(r.heads_in[0, place, :], r.heads_in[1, :span, :], 1, 1) * score_scale
                query_at = (base + step) * tokens + lax.broadcasted_iota(jnp.int32, (tokens, span), 0)
                key_at = lax.broadcasted_iota(jnp.int32, (tokens, span), 1)
                same = (query_at // BLK == key_at // BLK) & (key_at <= query_at)
                bias = jnp.concatenate(
                    [
                        jnp.broadcast_to(r.bias[pl.ds((base + step) * sub + line, 1), :span], (BLK, span))
                        for line in range(sub)
                    ],
                    axis=0,
                )
                scores = scores + jnp.where(same, 0.0, bias)
                top = jnp.max(scores, axis=1, keepdims=True)
                weight = jnp.exp(scores - top)
                weight = weight / jnp.sum(weight, axis=1, keepdims=True)
                r.probs[place, :span] = weight.astype(low)
                r.probs_turned[:span, place] = weight.T.astype(low)
                return carry

            lax.fori_loop(0, group, body, 0)

        for base in range(0, seq_count, group):
            forward(base)
        turn_weights(3, 4)

        def turned_back(values, place):
            return (
                values * r.cosine[place, :]
                - pltpu.roll(values, HEAD_DIM // 2, 1) * r.sine[place, :]
            ).astype(low)

        def grad_rows(term, first, count):
            if term == 0:
                return r.heads_in[3, pl.ds(first * tokens, count * tokens), :]
            block = r.late_in[term - 1, pl.ds(first * tensor_count, count * tensor_count)]
            return block.reshape(count * tokens, HEAD_DIM)

        def backward(term):
            r.key_acc[...] = jnp.zeros(r.key_acc.shape, full)
            for base in range(0, seq_count, group):
                later = slice(base * tokens, length)
                for step in range(group):
                    place = slice((base + step) * tokens, (base + step + 1) * tokens)
                    r.grads_out[2 * term + 1, place, :] = product(
                        r.probs_turned[place, later],
                        grad_rows(term, base, seq_count - base),
                        1,
                        0,
                    ).astype(low)
            grads_start(2 * term + 1)

            def at(base):
                span = (base + group) * tokens

                def body(step, carry):
                    at_block = base + group - 1 - step
                    place = window(at_block, tokens)
                    probs = r.probs[place, :span]
                    grad_low = grad_rows(term, at_block, 1)
                    grad_probs = product(grad_low, r.heads_in[2, :span, :], 1, 1)
                    wide = probs.astype(full)
                    delta = jnp.sum(wide * grad_probs, axis=1, keepdims=True)
                    grad_scores = (wide * (grad_probs - delta)).astype(low)
                    grad_query = product(grad_scores, r.heads_in[1, :span, :], 1, 0) * score_scale
                    r.query_out[term, window(at_block, tensor_count)] = turned_back(
                        grad_query, place
                    ).reshape(tensor_count, HALVES, lines, HEAD_DIM)
                    r.key_acc[:span, :] += product(grad_scores, r.heads_in[0, place, :], 0, 0)
                    return carry

                lax.fori_loop(0, group, body, 0)

            for base in reversed(range(0, seq_count, group)):
                at(base)
            r.grads_out[2 * term] = turned_back(r.key_acc[...] * score_scale, slice(None))
            grads_start(2 * term)
            query_start(term)

        def hand_on(term, half, chunk):
            place = window(chunk, part)
            hand_copy(term, half, chunk).wait_recv()
            gain_term = jnp.zeros((1, part), full)
            for step in range(chips):
                owner = 2 * lax.rem(chip + step, chips) + core
                handed = r.hand_in[term, half, step, :, place].astype(full)
                pair = r.total[owner, half, :, place] + handed
                if step:
                    r.far_out[term, half, step - 1, :, place] = pair.astype(low)
                    far_copy(term, half, step, chunk).start()
                else:
                    r.normed_grad[half, :, place] = pair
                gain_term += jnp.sum(pair * r.scaled[step, half, :, place], axis=0, keepdims=True)
            if term + half:
                gain_term += r.gain_sum[:, place]
            if term < ITERS - 1 or half < HALVES - 1:
                r.gain_sum[:, place] = gain_term
                return
            r.gain_own[window(chunk, gain_part), :] = jnp.concatenate(
                [gain_term[:, line * HEAD_DIM : (line + 1) * HEAD_DIM] for line in range(gain_part)],
                axis=0,
            )
            for mask in order:
                wide_copy(mask, chunk).start()

        def push(term):
            for item in (1, 0):
                grads_ready(2 * term + item)

                def body(chunk, carry):
                    place = window(chunk, part)
                    weight = r.weights[block_of(1 - item, chunk)]
                    value = product(r.grads_in[2 * term + item], weight, 1, 0)
                    value = value.reshape(tensor_count, HALVES, lines, part)
                    if item == 0:
                        value = value + r.total[:, :, :, place]
                    r.total[:, :, :, place] = value
                    return carry

                lax.fori_loop(0, CHUNKS, body, 0)
            for half in range(HALVES):
                query_whole(term, half).wait_recv()

                def last(chunk, carry):
                    place = window(chunk, part)
                    grads = r.query_in[term, half].reshape(half_tokens, head_width)
                    value = product(grads, r.weights[block_of(2, chunk)], 1, 0)
                    r.total[:, half, :, place] += value.reshape(tensor_count, lines, part)
                    for step in range(chips):
                        other = 2 * lax.rem(chip + step, chips) + 1 - core
                        r.hand_out[term, half, step, :, place] = r.total[
                            other, half, :, place
                        ].astype(low)
                    hand_copy(term, half, chunk).start()

                    @pl.when(chunk > 0)
                    def _():
                        hand_on(term, half, chunk - 1)

                    if half:

                        @pl.when(chunk == 0)
                        def _():
                            hand_on(term, half - 1, CHUNKS - 1)

                    return carry

                lax.fori_loop(0, CHUNKS, last, 0)
            hand_on(term, HALVES - 1, CHUNKS - 1)

        def finish(term, half):
            for chunk in range(CHUNKS):
                place = slice(chunk * part, (chunk + 1) * part)
                far_ready(term, half, chunk)
                value = r.normed_grad[half, :, place]
                for step in range(1, chips):
                    value = value + r.far_in[term, half, step - 1, :, place].astype(full)
                r.normed_grad[half, :, place] = value
            scaled = r.scaled[0, half]
            weighted = r.gain[...] * r.normed_grad[half]
            inner = jnp.sum(weighted * scaled, axis=1, keepdims=True)
            cotangent = inv_rms[half] * (weighted - scaled * (inner / width))
            if term == 0:
                adjoint_out[half] = cotangent
            else:
                adjoint_out[half] += cotangent
            if term < ITERS - 1:
                r.series[term, half, me] = cotangent.astype(low)
                gather_start((term + 1, half))

        for term in range(ITERS):
            if term:
                r.total[:, :, :, :head_width] = jnp.zeros(spread_rows, full)
                for half in range(HALVES):
                    gather_each((term, half), pull(term, half))
                    late_start(term, half)
                for half in range(HALVES):
                    late_whole(term, half).wait_recv()
            else:
                heads_ready(2)
                heads_ready(3)
            backward(term)
            push(term)
            for half in range(HALVES):
                finish(term, half)

        for item in range(2):
            gather_drain(item)
        for item in range(4):
            heads_drain(item)
        for item in range(2 * ITERS):
            grads_drain(item)
        for term in range(ITERS):
            for half in range(HALVES):
                query_whole(term, half).wait_send()
                if term:
                    gather_drain((term, half))
                    late_whole(term, half).wait_send()
        for term in range(ITERS):
            reduce_drain(term)
        block = r.gain_far.at[pl.ds(1, seq_count - 1)]
        remote(
            block, block, r.wide_send.at[0], r.wide_recv.at[0], "seq", flipped(me_seq, 1, bits)
        ).wait()
        value = r.gain_own[...]
        for mask in order:
            value = value + r.gain_far[mask]
        r.gain_mid[...] = value
        for step in range(1, tensor_count):
            near_copy(step).start()
        block = r.gain_near.at[pl.ds(1, tensor_count - 1)]
        remote(block, block, r.near_send.at[0], r.near_recv.at[0], "tensor", partner).wait()
        for step in range(1, tensor_count):
            value = value + r.gain_near[step]
        gain_out[...] = value

    anywhere = pl.BlockSpec(memory_space=pl.ANY)
    adjoint, gain_grad = pl.pallas_call(
        kernel,
        out_shape=[
            jax.ShapeDtypeStruct((HALVES, lines, width), full),
            jax.ShapeDtypeStruct((gain_rows, HEAD_DIM), full),
        ],
        in_specs=[anywhere] * 10,
        out_specs=[pl.BlockSpec(memory_space=pltpu.VMEM)] * 2,
        scratch_shapes=list(scratch.values()),
        compiler_params=pltpu.CompilerParams(
            collective_id=0, has_side_effects=True, vmem_limit_bytes=58 << 20
        ),
    )(
        fixed_point.reshape(HALVES, lines, width),
        incoming,
        norm_gain.reshape(1, width),
        query_weight.reshape(CHUNKS, part, head_width),
        key_weight.reshape(CHUNKS, part, head_width),
        value_weight.reshape(CHUNKS, part, head_width),
        out_weight,
        layout,
        jnp.asarray(cosine),
        jnp.asarray(sine),
    )
    adjoint = incoming.astype(full) + adjoint.reshape(rows, width)
    return adjoint, gain_grad.reshape(width) * length ** (-0.5)


def solution(mesh):
    in_specs = (
        P(("seq", "tensor"), None),
        P(("seq", "tensor"), None),
        P(),
        P(None, "tensor"),
        P(None, "tensor"),
        P(None, "tensor"),
        P("tensor", None),
        P(),
    )
    out_specs = (P(("seq", "tensor"), None), P())
    seq, tensor = mesh.shape["seq"], mesh.shape["tensor"]

    def body(*arrays):
        heads = arrays[3].shape[1] * tensor // HEAD_DIM
        tokens = arrays[0].shape[0] * tensor
        fits = (
            tensor % 2 == 0
            and tensor >= 4
            and seq & (seq - 1) == 0
            and heads == seq * tensor
            and tokens % 128 == 0
            and arrays[0].shape[0] % (16 * HALVES) == 0
            and arrays[0].shape[1] == CHUNKS * arrays[3].shape[1]
            and arrays[3].shape[1] % (8 * HEAD_DIM) == 0
        )
        return (fused_body if fits else ring_body)(*arrays)

    return jax.shard_map(body, mesh=mesh, in_specs=in_specs, out_specs=out_specs, check_vma=False)
```

```python
import types

import jax
import jax.numpy as jnp
import numpy as np
from jax import lax
from jax.experimental import pallas as pl
from jax.experimental.pallas import tpu as pltpu
from jax.sharding import PartitionSpec as P

HEAD_DIM = 128
BLK = 64
ITERS = 2


EPS = 1e-05
THETA = 10000.0
MASKED = -1e30


def rope_tables(positions):
    freq = THETA ** (-jnp.arange(0, HEAD_DIM, 2, dtype=jnp.float32) / HEAD_DIM)
    angle = positions.astype(jnp.float32)[:, None] * freq[None, :]
    cosine = jnp.concatenate([jnp.cos(angle), jnp.cos(angle)], axis=1)[:, None, :]
    sine = jnp.concatenate([jnp.sin(angle), jnp.sin(angle)], axis=1)[:, None, :]
    return (cosine, sine)


def rotate(values, cosine, sine):
    half = HEAD_DIM // 2
    turned = jnp.concatenate([-values[..., half:], values[..., :half]], axis=-1)
    return values * cosine + turned * sine


def rotate_back(values, cosine, sine):
    half = HEAD_DIM // 2
    weighted = values * sine
    turned = jnp.concatenate([weighted[..., half:], -weighted[..., :half]], axis=-1)
    return values * cosine + turned


def expand_blocks(chosen):
    return jnp.repeat(jnp.repeat(chosen, BLK, axis=0), BLK, axis=1)


def pair_mask(query_pos, key_pos, chosen):
    query_block = (query_pos // BLK)[:, None]
    key_block = (key_pos // BLK)[None, :]
    earlier = (key_block < query_block) & chosen
    same = (key_block == query_block) & (key_pos[None, :] <= query_pos[:, None])
    return earlier | same


def ring_body(
    fixed_point, incoming, norm_gain, query_weight, key_weight, value_weight, out_weight, layout
):
    local_rows, model_width = fixed_point.shape
    head_width = query_weight.shape[1]
    head_count = head_width // HEAD_DIM
    seq_tokens = local_rows * lax.axis_size("tensor")
    seq_length = seq_tokens * lax.axis_size("seq")
    seq_index = lax.axis_index("seq")
    score_scale = HEAD_DIM ** (-0.5)
    contract_last = (((1,), (1,)), ((), ()))
    head_shape = (seq_tokens, head_count, HEAD_DIM)
    point = fixed_point.astype(jnp.float32)
    inv_rms = lax.rsqrt(jnp.mean(point * point, axis=1, keepdims=True) + EPS)
    scaled = point * inv_rms
    normed = (norm_gain * scaled).astype(jnp.bfloat16)
    project_piece = lax.all_gather(normed, "tensor", axis=0, tiled=True)
    projected = jnp.concatenate(
        [
            jnp.dot(project_piece, query_weight, preferred_element_type=jnp.float32),
            jnp.dot(project_piece, key_weight, preferred_element_type=jnp.float32),
            jnp.dot(project_piece, value_weight, preferred_element_type=jnp.float32),
        ],
        axis=1,
    )
    positions = seq_index * seq_tokens + jnp.arange(seq_tokens, dtype=jnp.int32)
    cosine, sine = rope_tables(positions)
    queries = rotate(projected[:, :head_width].reshape(head_shape), cosine, sine).astype(
        jnp.bfloat16
    )
    keys = rotate(
        projected[:, head_width : 2 * head_width].reshape(head_shape), cosine, sine
    ).astype(jnp.bfloat16)
    values = projected[:, 2 * head_width :].reshape(head_shape).astype(jnp.bfloat16)
    block_rows = seq_tokens // BLK
    block_count = seq_length // BLK
    first_block = seq_index * block_rows
    key_positions = jnp.arange(seq_length, dtype=jnp.int32)
    chosen_rows = (
        lax.dynamic_slice(layout, (first_block, jnp.int32(0)), (block_rows, block_count)) > 0
    )
    allowed = pair_mask(positions, key_positions, expand_blocks(chosen_rows))
    keys_all, values_all = (
        lax.all_gather(keys, "seq", axis=0, tiled=True),
        lax.all_gather(values, "seq", axis=0, tiled=True),
    )
    scores = (
        jnp.einsum("qhd,khd->hqk", queries, keys_all, preferred_element_type=jnp.float32)
        * score_scale
    )
    scores = jnp.where(allowed[None], scores, MASKED)
    log_norm = jax.nn.logsumexp(scores, axis=2, keepdims=True)
    probs = jnp.exp(scores - log_norm)
    probs_low = probs.astype(jnp.bfloat16)
    attended = jnp.einsum(
        "hqk,khd->qhd", probs_low, values_all, preferred_element_type=jnp.float32
    ).astype(jnp.bfloat16)
    cotangent = incoming.astype(jnp.float32)
    adjoint = cotangent
    gain_grad = jnp.zeros((model_width,), jnp.float32)
    for term_index in range(ITERS):
        grad_out = lax.dot_general(
            lax.all_gather(cotangent.astype(jnp.bfloat16), "tensor", axis=0, tiled=True),
            out_weight,
            contract_last,
            preferred_element_type=jnp.float32,
        )
        grad_low = grad_out.astype(jnp.bfloat16).reshape(head_shape)
        delta = jnp.sum(grad_low.astype(jnp.float32) * attended.astype(jnp.float32), axis=2)
        grad_probs = jnp.einsum(
            "qhd,khd->hqk", grad_low, values_all, preferred_element_type=jnp.float32
        )
        grad_scores = (probs * (grad_probs - delta.T[:, :, None])).astype(jnp.bfloat16)
        grad_query = (
            jnp.einsum("hqk,khd->qhd", grad_scores, keys_all, preferred_element_type=jnp.float32)
            * score_scale
        )
        key_part = (
            jnp.einsum("hqk,qhd->khd", grad_scores, queries, preferred_element_type=jnp.float32)
            * score_scale
        )
        value_part = jnp.einsum(
            "hqk,qhd->khd", probs_low, grad_low, preferred_element_type=jnp.float32
        )
        key_grads = lax.psum_scatter(
            jnp.concatenate(
                [
                    key_part.reshape(seq_tokens * lax.axis_size("seq"), head_width),
                    value_part.reshape(seq_tokens * lax.axis_size("seq"), head_width),
                ],
                axis=1,
            ).astype(jnp.bfloat16),
            "seq",
            scatter_dimension=0,
            tiled=True,
        ).astype(jnp.float32)
        grad_key = key_grads[:, :head_width].reshape(head_shape)
        grad_value = key_grads[:, head_width:].reshape(head_shape)
        query_low = (
            rotate_back(grad_query, cosine, sine)
            .astype(jnp.bfloat16)
            .reshape(seq_tokens, head_width)
        )
        key_low = (
            rotate_back(grad_key, cosine, sine).astype(jnp.bfloat16).reshape(seq_tokens, head_width)
        )
        value_low = grad_value.astype(jnp.bfloat16).reshape(seq_tokens, head_width)
        total = lax.dot_general(
            query_low, query_weight, contract_last, preferred_element_type=jnp.float32
        )
        total = total + lax.dot_general(
            key_low, key_weight, contract_last, preferred_element_type=jnp.float32
        )
        total = total + lax.dot_general(
            value_low, value_weight, contract_last, preferred_element_type=jnp.float32
        )
        grad_normed = lax.psum_scatter(
            total.astype(jnp.bfloat16), "tensor", scatter_dimension=0, tiled=True
        ).astype(jnp.float32)
        gain_term = jnp.sum(grad_normed * scaled, axis=0)
        gain_grad = gain_grad + lax.psum(gain_term, ("seq", "tensor"))
        weighted = norm_gain * grad_normed
        inner = jnp.sum(weighted * scaled, axis=1, keepdims=True)
        cotangent = inv_rms * (weighted - scaled * (inner / model_width))
        adjoint = adjoint + cotangent
    return (adjoint, gain_grad * seq_length ** (-0.5))


CHUNKS = 4
HALVES = 2
LAG = 2
MESH = pl.DeviceIdType.MESH


def numpy_tables(length):
    freq = np.float32(THETA) ** (-np.arange(0, HEAD_DIM, 2, dtype=np.float32) / np.float32(HEAD_DIM))
    angle = np.arange(length, dtype=np.float32)[:, None] * freq.astype(np.float32)[None, :]
    cosine = np.cos(angle.astype(np.float64)).astype(np.float32)
    sine = np.sin(angle.astype(np.float64)).astype(np.float32)
    return np.concatenate([cosine, cosine], axis=1), np.concatenate([-sine, sine], axis=1)


def product(left, right, left_dim, right_dim):
    return lax.dot_general(
        left, right, (((left_dim,), (right_dim,)), ((), ())), preferred_element_type=jnp.float32
    )


def flipped(index, mask, bits):
    result = 0
    for bit in range(bits):
        here = lax.rem(lax.div(index, 1 << bit), 2)
        result = result + (1 << bit) * ((1 - here) if (mask >> bit) & 1 else here)
    return result


def window(index, size):
    return pl.ds(pl.multiple_of(index * size, size), size)


def fused_body(
    fixed_point, incoming, norm_gain, query_weight, key_weight, value_weight, out_weight, layout
):
    rows, width = fixed_point.shape
    tensor_count = lax.axis_size("tensor")
    seq_count = lax.axis_size("seq")
    chips = tensor_count // 2
    bits = seq_count.bit_length() - 1
    head_width = query_weight.shape[1]
    tokens = rows * tensor_count
    length = tokens * seq_count
    blocks = layout.shape[0]
    part = width // CHUNKS
    lines = rows // HALVES
    groups = length // rows
    half_tokens = tensor_count * lines
    score_scale = HEAD_DIM ** (-0.5)
    gain_rows = width // HEAD_DIM
    gain_part = gain_rows // CHUNKS
    cosine, sine = numpy_tables(length)
    order = list(range(seq_count - 1, 0, -1))
    low, full = jnp.bfloat16, jnp.float32
    dma = pltpu.SemaphoreType.DMA
    scratch = {
        "weights": pltpu.VMEM((4 * CHUNKS + 1, part, head_width), low),
        "inverse": pltpu.VMEM((tokens, HEAD_DIM), full),
        "gain": pltpu.VMEM((1, width), full),
        "layout": pltpu.VMEM(layout.shape, jnp.int32),
        "cosine": pltpu.VMEM((length, HEAD_DIM), full),
        "sine": pltpu.VMEM((length, HEAD_DIM), full),
        "bias": pltpu.VMEM((blocks, length), full),
        "scaled": pltpu.VMEM((HALVES, lines, width), full),
        "pieces": pltpu.VMEM((3, tokens, width), low),
        "series": pltpu.VMEM((ITERS - 1, HALVES, tensor_count, lines, width), low),
        "heads_out": pltpu.VMEM((4, seq_count, tokens, HEAD_DIM), low),
        "heads_in": pltpu.VMEM((4, length, HEAD_DIM), low),
        "late_out": pltpu.VMEM(
            (ITERS - 1, HALVES, seq_count, tensor_count, lines, HEAD_DIM), low
        ),
        "late_in": pltpu.VMEM((ITERS - 1, groups, HALVES, lines, HEAD_DIM), low),
        "probs": pltpu.VMEM((length, length), low),
        "key_acc": pltpu.VMEM((length, HEAD_DIM), full),
        "probs_turned": pltpu.VMEM((length, length), low),
        "grads_out": pltpu.VMEM((2 * ITERS, length, HEAD_DIM), low),
        "grads_in": pltpu.VMEM((2 * ITERS, tokens, head_width), low),
        "query_out": pltpu.VMEM((ITERS, groups, HALVES, lines, HEAD_DIM), low),
        "query_in": pltpu.VMEM((ITERS, HALVES, tensor_count, lines, head_width), low),
        "total": pltpu.VMEM((tensor_count, HALVES, lines, width), full),
        "hand_out": pltpu.VMEM((ITERS, HALVES, chips, lines, width), low),
        "hand_in": pltpu.VMEM((ITERS, HALVES, chips, lines, width), low),
        "far_out": pltpu.VMEM((ITERS, HALVES, chips - 1, lines, width), low),
        "far_in": pltpu.VMEM((ITERS, HALVES, chips - 1, lines, width), low),
        "normed_grad": pltpu.VMEM((HALVES, lines, width), full),
        "gain_sum": pltpu.VMEM((1, width), full),
        "gain_own": pltpu.VMEM((gain_rows, HEAD_DIM), full),
        "gain_near": pltpu.VMEM((tensor_count, gain_rows, HEAD_DIM), full),
        "gain_mid": pltpu.VMEM((gain_rows, HEAD_DIM), full),
        "gain_far": pltpu.VMEM((seq_count, gain_rows, HEAD_DIM), full),
        "load_sem": dma((6,)),
        "weight_sem": dma((CHUNKS + 1,)),
        "gather_send": dma((3,)),
        "gather_far": dma((3, CHUNKS * (chips - 1))),
        "gather_near": dma((3, CHUNKS)),
        "series_send": dma(((ITERS - 1) * HALVES,)),
        "series_far": dma(((ITERS - 1) * HALVES, CHUNKS * (chips - 1))),
        "series_near": dma(((ITERS - 1) * HALVES, CHUNKS)),
        "heads_send": dma((4,)),
        "heads_recv": dma((4,)),
        "late_send": dma(((ITERS - 1) * HALVES,)),
        "late_recv": dma(((ITERS - 1) * HALVES,)),
        "grads_send": dma((2 * ITERS,)),
        "grads_recv": dma((2 * ITERS,)),
        "query_send": dma((ITERS * HALVES,)),
        "query_recv": dma((ITERS * HALVES,)),
        "hand_send": dma((ITERS,)),
        "hand_recv": dma((ITERS * HALVES, CHUNKS)),
        "far_send": dma((ITERS,)),
        "far_recv": dma((ITERS * HALVES, CHUNKS)),
        "near_send": dma((1,)),
        "near_recv": dma((1,)),
        "wide_send": dma((1,)),
        "wide_recv": dma((1,)),
    }

    def kernel(*refs):
        point_hbm, incoming_hbm, gain_hbm, wq_hbm, wk_hbm, wv_hbm, wo_hbm = refs[:7]
        layout_hbm, cosine_hbm, sine_hbm, adjoint_out, gain_out = refs[7:12]
        r = types.SimpleNamespace(**dict(zip(scratch, refs[12:])))
        me_seq = lax.axis_index("seq")
        me = lax.axis_index("tensor")
        core = lax.rem(me, 2)
        chip = lax.div(me, 2)
        partner = me + 1 - 2 * core
        own_rows = window(me, rows)
        own_tokens = window(me_seq, tokens)
        own_columns = window(me_seq, HEAD_DIM)

        barrier = pltpu.get_barrier_semaphore()
        for step in range(1, tensor_count):
            pl.semaphore_signal(
                barrier,
                inc=1,
                device_id={"tensor": lax.rem(me + step, tensor_count)},
                device_id_type=MESH,
            )
        for mask in order:
            pl.semaphore_signal(
                barrier,
                inc=1,
                device_id={"seq": flipped(me_seq, mask, bits)},
                device_id_type=MESH,
            )

        def load(index, source, target):
            return pltpu.make_async_copy(source, target, r.load_sem.at[index])

        loads = [
            load(0, point_hbm, r.pieces.at[2, own_rows, :]),
            load(1, gain_hbm, r.gain),
            load(2, incoming_hbm, r.pieces.at[1, own_rows, :]),
            load(3, layout_hbm, r.layout),
            load(4, cosine_hbm, r.cosine),
            load(5, sine_hbm, r.sine),
        ]
        for index in (0, 1, 2, 3):
            loads[index].start()

        def block_of(item, chunk):
            return item * CHUNKS + chunk

        def weight_load(item, chunk):
            if item == 3:
                source = wo_hbm.at[:, window(chunk, part)]
            else:
                source = (wv_hbm, wk_hbm, wq_hbm)[item].at[chunk]
            target = r.weights.at[1 + block_of(item, chunk)]
            return pltpu.make_async_copy(
                source, target, r.weight_sem.at[CHUNKS if item == 3 else chunk]
            )

        def weight_ready(index, count):
            pltpu.make_async_copy(
                wq_hbm.at[pl.ds(0, count)], r.weights.at[pl.ds(0, count)], r.weight_sem.at[index]
            ).wait()

        def turn_weights(first, last):
            def body(block, carry):
                for line in range(0, part, HEAD_DIM):
                    strip = slice(line, line + HEAD_DIM)
                    r.weights[block, :, strip] = r.weights[block + 1, strip, :].T
                return carry

            lax.fori_loop(first * CHUNKS, last * CHUNKS, body, 0)

        def remote(source, target, send, recv, axis, peer):
            return pltpu.make_async_remote_copy(
                src_ref=source,
                dst_ref=target,
                send_sem=send,
                recv_sem=recv,
                device_id={axis: peer},
                device_id_type=MESH,
            )

        def gather_parts(item, chunk, origin):
            place = window(chunk, part)
            if isinstance(item, tuple):
                term, half = item
                index = (term - 1) * HALVES + half
                block = r.series.at[term - 1, half, origin, :, place]
                return block, r.series_send.at[index], r.series_far, r.series_near, index
            block = r.pieces.at[item, window(origin, rows), place]
            return block, r.gather_send.at[item], r.gather_far, r.gather_near, item

        def gather_far(item, chunk, step):
            block, send, far, near, index = gather_parts(item, chunk, me)
            recv = far.at[index, chunk * (chips - 1) + step - 1]
            peer = 2 * lax.rem(chip + step, chips) + core
            return remote(block, block, send, recv, "tensor", peer)

        def gather_near(item, chunk):
            block, send, far, near, index = gather_parts(item, chunk, me)
            return remote(block, block, send, near.at[index, chunk], "tensor", partner)

        def gather_pass(item, chunk, step):
            origin = 2 * lax.rem(chip + chips - step, chips) + core
            block, send, far, near, index = gather_parts(item, chunk, origin)
            return remote(block, block, send, near.at[index, chunk], "tensor", partner)

        def gather_start(item):
            for chunk in range(CHUNKS):
                for step in range(1, chips):
                    gather_far(item, chunk, step).start()
                gather_near(item, chunk).start()

        def gather_relay(item, chunk):
            for step in range(1, chips):
                gather_far(item, chunk, step).wait_recv()
                gather_pass(item, chunk, step).start()

        def gather_ready(item, chunk):
            place = window(chunk, part)
            block, send, far, near, index = gather_parts(item, chunk, 0)
            if isinstance(item, tuple):
                block = r.series.at[item[0] - 1, item[1], pl.ds(0, chips), :, place]
            else:
                block = r.pieces.at[item, pl.ds(0, chips * rows), place]
            remote(block, block, send, near.at[index, chunk], "tensor", partner).wait_recv()

        def gather_drain(item):
            block, send, far, near, index = gather_parts(item, 0, 0)
            if isinstance(item, tuple):
                block = r.series.at[item[0] - 1, item[1], pl.ds(0, 2 * chips - 1)]
            else:
                block = r.pieces.at[item, pl.ds(0, (2 * chips - 1) * rows), :]
            remote(block, block, send, near.at[index, 0], "tensor", partner).wait_send()

        def gather_each(item, use, after=None, count=CHUNKS):
            gather_relay(item, 0)

            def body(chunk, carry):
                @pl.when(chunk + 1 < CHUNKS)
                def _():
                    gather_relay(item, chunk + 1)

                if after is not None:

                    @pl.when(chunk + 2 == CHUNKS)
                    def _():
                        after()

                gather_ready(item, chunk)
                use(chunk)
                return carry

            lax.fori_loop(0, count, body, 0)

        def columns_of(slot):
            return slice(slot * head_width, (slot + 1) * head_width)

        def heads_copy(item, mask):
            return remote(
                r.heads_out.at[item, mask],
                r.heads_in.at[item, own_tokens, :],
                r.heads_send.at[item],
                r.heads_recv.at[item],
                "seq",
                flipped(me_seq, mask, bits),
            )

        def heads_start(item, turn):
            for mask in order + [0]:
                peer = flipped(me_seq, mask, bits)
                columns = window(item * seq_count + peer, HEAD_DIM)
                values = r.total[:, :, :, columns].reshape(tokens, HEAD_DIM)
                if turn:
                    values = (
                        values * r.cosine[own_tokens, :]
                        + pltpu.roll(values, HEAD_DIM // 2, 1) * r.sine[own_tokens, :]
                    )
                if mask:
                    r.heads_out[item, mask] = values.astype(low)
                else:
                    r.heads_in[item, own_tokens, :] = values.astype(low)
            for mask in order:
                heads_copy(item, mask).start()

        def late_copy(term, half, mask):
            index = (term - 1) * HALVES + half
            return remote(
                r.late_out.at[term - 1, half, mask],
                r.late_in.at[term - 1, window(me_seq, tensor_count), half],
                r.late_send.at[index],
                r.late_recv.at[index],
                "seq",
                flipped(me_seq, mask, bits),
            )

        def late_start(term, half):
            for mask in order + [0]:
                columns = window(flipped(me_seq, mask, bits), HEAD_DIM)
                values = r.total[:, half, :, columns].astype(low)
                if mask:
                    r.late_out[term - 1, half, mask] = values
                else:
                    r.late_in[term - 1, window(me_seq, tensor_count), half] = values
            for mask in order:
                late_copy(term, half, mask).start()

        def late_whole(term, half):
            block = r.late_out.at[term - 1, half, pl.ds(1, seq_count - 1)]
            index = (term - 1) * HALVES + half
            send, recv = r.late_send.at[index], r.late_recv.at[index]
            return remote(block, block, send, recv, "seq", flipped(me_seq, 1, bits))

        def heads_ready(item):
            block = r.heads_in.at[item, pl.ds(0, (seq_count - 1) * tokens), :]
            send, recv = r.heads_send.at[item], r.heads_recv.at[item]
            remote(block, block, send, recv, "seq", flipped(me_seq, 1, bits)).wait_recv()

        def heads_drain(item):
            block = r.heads_out.at[item, pl.ds(1, seq_count - 1)]
            send, recv = r.heads_send.at[item], r.heads_recv.at[item]
            remote(block, block, send, recv, "seq", flipped(me_seq, 1, bits)).wait_send()

        def grads_copy(item, mask):
            peer = flipped(me_seq, mask, bits)
            return remote(
                r.grads_out.at[item, window(peer, tokens), :],
                r.grads_in.at[item, :, own_columns],
                r.grads_send.at[item],
                r.grads_recv.at[item],
                "seq",
                peer,
            )

        def grads_start(item):
            for mask in order:
                grads_copy(item, mask).start()
            r.grads_in[item, :, own_columns] = r.grads_out[item, own_tokens, :]

        def grads_ready(item):
            block = r.grads_in.at[item, :, pl.ds(0, (seq_count - 1) * HEAD_DIM)]
            send, recv = r.grads_send.at[item], r.grads_recv.at[item]
            remote(block, block, send, recv, "seq", flipped(me_seq, 1, bits)).wait_recv()

        def grads_drain(item):
            block = r.grads_out.at[item, pl.ds(0, (seq_count - 1) * tokens), :]
            send, recv = r.grads_send.at[item], r.grads_recv.at[item]
            remote(block, block, send, recv, "seq", flipped(me_seq, 1, bits)).wait_send()

        def query_copy(term, half, mask):
            peer = flipped(me_seq, mask, bits)
            index = term * HALVES + half
            return remote(
                r.query_out.at[term, window(peer, tensor_count), half],
                r.query_in.at[term, half, :, :, own_columns],
                r.query_send.at[index],
                r.query_recv.at[index],
                "seq",
                peer,
            )

        def query_start(term):
            for half in range(HALVES):
                for mask in order:
                    query_copy(term, half, mask).start()
                own = r.query_out[term, window(me_seq, tensor_count), half]
                r.query_in[term, half, :, :, own_columns] = own

        def query_whole(term, half):
            block = r.query_in.at[term, half, :, :, pl.ds(0, (seq_count - 1) * HEAD_DIM)]
            index = term * HALVES + half
            send, recv = r.query_send.at[index], r.query_recv.at[index]
            return remote(block, block, send, recv, "seq", flipped(me_seq, 1, bits))

        def hand_copy(term, half, chunk):
            place = window(chunk, part)
            return remote(
                r.hand_out.at[term, half, :, :, place],
                r.hand_in.at[term, half, :, :, place],
                r.hand_send.at[term],
                r.hand_recv.at[term * HALVES + half, chunk],
                "tensor",
                partner,
            )

        def far_copy(term, half, step, chunk):
            place = window(chunk, part)
            return remote(
                r.far_out.at[term, half, step - 1, :, place],
                r.far_in.at[term, half, step - 1, :, place],
                r.far_send.at[term],
                r.far_recv.at[term * HALVES + half, chunk],
                "tensor",
                2 * lax.rem(chip + step, chips) + core,
            )

        def far_ready(term, half, chunk):
            block = r.far_in.at[term, half, :, :, window(chunk, part)]
            send, recv = r.far_send.at[term], r.far_recv.at[term * HALVES + half, chunk]
            remote(block, block, send, recv, "tensor", partner).wait_recv()

        def reduce_drain(term):
            block = r.hand_out.at[term]
            send, recv = r.hand_send.at[term], r.hand_recv.at[term * HALVES, 0]
            remote(block, block, send, recv, "tensor", partner).wait_send()
            block = r.far_out.at[term]
            send, recv = r.far_send.at[term], r.far_recv.at[term * HALVES, 0]
            remote(block, block, send, recv, "tensor", partner).wait_send()

        def wide_copy(mask, chunk):
            place = window(chunk, gain_part)
            return remote(
                r.gain_own.at[place, :],
                r.gain_far.at[mask, place, :],
                r.wide_send.at[0],
                r.wide_recv.at[0],
                "seq",
                flipped(me_seq, mask, bits),
            )

        def near_copy(step):
            return remote(
                r.gain_mid,
                r.gain_near.at[step],
                r.near_send.at[0],
                r.near_recv.at[0],
                "tensor",
                lax.rem(me + step, tensor_count),
            )

        for copy in loads[:3]:
            copy.wait()
        for chunk in range(CHUNKS):
            for item in range(3):
                weight_load(item, chunk).start()
        for chunk in range(CHUNKS):
            weight_load(3, chunk).start()
        for copy in loads[4:]:
            copy.start()

        point = r.pieces[2, own_rows, :].astype(full).reshape(HALVES, lines, width)
        inv_rms = lax.rsqrt(jnp.mean(point * point, axis=-1, keepdims=True) + EPS)
        r.scaled[...] = point * inv_rms
        normed = r.gain[...].reshape(1, 1, width) * r.scaled[...]
        r.pieces[0, own_rows, :] = normed.astype(low).reshape(rows, width)
        pl.semaphore_wait(barrier, tensor_count - 1 + seq_count - 1)
        gather_start(0)

        loads[3].wait()
        spread = (
            lax.broadcasted_iota(jnp.int32, (blocks, length), 1) // BLK
            == lax.broadcasted_iota(jnp.int32, (blocks, length), 0)
        )
        chosen = product(
            jnp.where(r.layout[...] > 0, 1.0, 0.0).astype(low),
            jnp.where(spread, 1.0, 0.0).astype(low),
            1,
            0,
        )
        earlier = (
            lax.broadcasted_iota(jnp.int32, (blocks, length), 1) // BLK
            < lax.broadcasted_iota(jnp.int32, (blocks, length), 0)
        )
        r.bias[...] = jnp.where(earlier & (chosen > 0.5), 0.0, MASKED)
        r.total[...] = jnp.zeros(r.total.shape, full)
        spread_rows = (tensor_count, HALVES, lines, head_width)

        def project_one(item, chunk):
            place = window(chunk, part)
            weight = r.weights[1 + block_of(2 - item, chunk)]
            value = product(r.pieces[0, :, place], weight, 1, 0)
            r.total[:, :, :, columns_of(item)] += value.reshape(spread_rows)

        def project(chunk):
            weight_ready(chunk, 3)
            for item in range(3):
                project_one(item, chunk)

        gather_each(0, project, lambda: gather_start(1), CHUNKS - 1)
        for copy in loads[4:]:
            copy.wait()
        gather_ready(0, CHUNKS - 1)
        weight_ready(CHUNKS - 1, 3)
        for item in range(3):
            project_one(item, CHUNKS - 1)
            heads_start(item, item < 2)
        weight_ready(CHUNKS, CHUNKS)

        def pull_first(chunk):
            place = window(chunk, part)
            weight = r.weights[1 + block_of(3, chunk)]
            value = product(r.pieces[1, :, place], weight, 1, 1)
            r.total[:, :, :, columns_of(3)] += value.reshape(spread_rows)

        gather_each(1, pull_first)
        heads_start(3, False)

        def pull(term, half):
            def use(chunk):
                place = window(chunk, part)
                piece = r.series[term - 1, half, :, :, place].reshape(half_tokens, part)
                value = product(piece, r.weights[block_of(3, chunk)], 1, 0)
                r.total[:, half, :, :head_width] += value.reshape(tensor_count, lines, head_width)

            return use
        gather_start(2)
        turn_weights(0, 3)

        for chunk in range(CHUNKS):
            gather_relay(2, chunk)
        for chunk in range(CHUNKS):
            gather_ready(2, chunk)

        group = 2 if seq_count % 2 == 0 else 1
        heads_ready(0)
        heads_ready(1)
        sub = tokens // BLK

        def forward(base):
            span = (base + group) * tokens

            def body(step, carry):
                place = window(base + step, tokens)
                scores = product(r.heads_in[0, place, :], r.heads_in[1, :span, :], 1, 1) * score_scale
                query_at = (base + step) * tokens + lax.broadcasted_iota(jnp.int32, (tokens, span), 0)
                key_at = lax.broadcasted_iota(jnp.int32, (tokens, span), 1)
                same = (query_at // BLK == key_at // BLK) & (key_at <= query_at)
                bias = jnp.concatenate(
                    [
                        jnp.broadcast_to(r.bias[pl.ds((base + step) * sub + line, 1), :span], (BLK, span))
                        for line in range(sub)
                    ],
                    axis=0,
                )
                scores = scores + jnp.where(same, 0.0, bias)
                top = jnp.max(scores, axis=1, keepdims=True)
                weight = jnp.exp(scores - top)
                weight = weight / jnp.sum(weight, axis=1, keepdims=True)
                r.probs[place, :span] = weight.astype(low)
                r.probs_turned[:span, place] = weight.T.astype(low)
                return carry

            lax.fori_loop(0, group, body, 0)

        for base in range(0, seq_count, group):
            forward(base)

        def turned_back(values, place):
            return (
                values * r.cosine[place, :]
                - pltpu.roll(values, HEAD_DIM // 2, 1) * r.sine[place, :]
            ).astype(low)

        def grad_rows(term, first, count):
            if term == 0:
                return r.heads_in[3, pl.ds(first * tokens, count * tokens), :]
            block = r.late_in[term - 1, pl.ds(first * tensor_count, count * tensor_count)]
            return block.reshape(count * tokens, HEAD_DIM)

        def backward(term):
            r.key_acc[...] = jnp.zeros(r.key_acc.shape, full)
            for base in range(0, seq_count, group):
                later = slice(base * tokens, length)
                for step in range(group):
                    place = slice((base + step) * tokens, (base + step + 1) * tokens)
                    r.grads_out[2 * term + 1, place, :] = product(
                        r.probs_turned[place, later],
                        grad_rows(term, base, seq_count - base),
                        1,
                        0,
                    ).astype(low)
            grads_start(2 * term + 1)

            def at(base):
                span = (base + group) * tokens

                def body(step, carry):
                    at_block = base + group - 1 - step
                    place = window(at_block, tokens)
                    probs = r.probs[place, :span]
                    grad_low = grad_rows(term, at_block, 1)
                    grad_probs = product(grad_low, r.heads_in[2, :span, :], 1, 1)
                    wide = probs.astype(full)
                    delta = jnp.sum(wide * grad_probs, axis=1, keepdims=True)
                    grad_scores = (wide * (grad_probs - delta)).astype(low)
                    grad_query = product(grad_scores, r.heads_in[1, :span, :], 1, 0) * score_scale
                    r.query_out[term, window(at_block, tensor_count)] = turned_back(
                        grad_query, place
                    ).reshape(tensor_count, HALVES, lines, HEAD_DIM)
                    r.key_acc[:span, :] += product(grad_scores, r.heads_in[0, place, :], 0, 0)
                    return carry

                lax.fori_loop(0, group, body, 0)

            for base in reversed(range(0, seq_count, group)):
                at(base)
            r.grads_out[2 * term] = turned_back(r.key_acc[...] * score_scale, slice(None))
            grads_start(2 * term)
            query_start(term)

        def hand_work(term, half, chunk):
            place = window(chunk, part)
            for step in range(chips):
                owner = 2 * lax.rem(chip + step, chips) + core
                handed = r.hand_in[term, half, step, :, place].astype(full)
                pair = r.total[owner, half, :, place] + handed
                if step:
                    r.far_out[term, half, step - 1, :, place] = pair.astype(low)
                else:
                    r.normed_grad[half, :, place] = pair

        def far_start(term, half, chunk):
            for step in range(1, chips):
                far_copy(term, half, step, chunk).start()

        def gain_on(term, half, chunk):
            place = window(chunk, part)
            gain_term = jnp.zeros((lines, part), full)
            for owner in range(tensor_count):
                own = slice(owner * rows + half * lines, owner * rows + (half + 1) * lines)
                scaled = r.pieces[2, own, place].astype(full) * r.inverse[own, :1]
                gain_term += r.total[owner, half, :, place] * scaled
            gain_term = jnp.sum(gain_term, axis=0, keepdims=True)
            if term + half:
                gain_term += r.gain_sum[:, place]
            if term < ITERS - 1 or half < HALVES - 1:
                r.gain_sum[:, place] = gain_term
                return
            r.gain_own[window(chunk, gain_part), :] = jnp.concatenate(
                [gain_term[:, line * HEAD_DIM : (line + 1) * HEAD_DIM] for line in range(gain_part)],
                axis=0,
            )
        def invert():
            for owner in range(tensor_count):
                place = slice(owner * rows, (owner + 1) * rows)
                point = r.pieces[2, place, :].astype(full)
                inverse = lax.rsqrt(jnp.mean(point * point, axis=1, keepdims=True) + EPS)
                r.inverse[place, :] = jnp.broadcast_to(inverse, (rows, HEAD_DIM))

        def push(term):
            if term == 0:
                invert()
            for item in (1, 0):
                if term == 0 and item == 0:
                    turn_weights(3, 4)
                grads_ready(2 * term + item)

                def body(chunk, carry):
                    place = window(chunk, part)
                    weight = r.weights[block_of(1 - item, chunk)]
                    value = product(r.grads_in[2 * term + item], weight, 1, 0)
                    value = value.reshape(tensor_count, HALVES, lines, part)
                    if item == 0:
                        value = value + r.total[:, :, :, place]
                    r.total[:, :, :, place] = value
                    return carry

                lax.fori_loop(0, CHUNKS, body, 0)

            def matmul(half, chunk):
                place = window(chunk, part)
                grads = r.query_in[term, half].reshape(half_tokens, head_width)
                value = product(grads, r.weights[block_of(2, chunk)], 1, 0)
                r.total[:, half, :, place] += value.reshape(tensor_count, lines, part)
                for step in range(chips):
                    other = 2 * lax.rem(chip + step, chips) + 1 - core
                    r.hand_out[term, half, step, :, place] = r.total[
                        other, half, :, place
                    ].astype(low)
                gain_on(term, half, chunk)

            def stage(half, first, last, behind):
                def body(chunk, carry):
                    if behind is not None:
                        earlier_half, shift = behind
                        hand_copy(term, earlier_half, chunk + shift).wait_recv()
                        hand_work(term, earlier_half, chunk + shift)
                        if term < ITERS - 1:
                            far_start(term, earlier_half, chunk + shift)
                    if half is not None:
                        matmul(half, chunk)
                        hand_copy(term, half, chunk).start()
                        if term == ITERS - 1 and half == HALVES - 1:
                            for mask in order:
                                wide_copy(mask, chunk).start()
                    if behind is not None and term == ITERS - 1:
                        far_start(term, earlier_half, chunk + shift)
                    return carry

                lax.fori_loop(first, last, body, 0)

            for half in range(HALVES):
                query_whole(term, half).wait_recv()
                stage(half, 0, LAG, (half - 1, CHUNKS - LAG) if half else None)
                stage(half, LAG, CHUNKS, (half, -LAG))
            stage(None, CHUNKS - LAG, CHUNKS, (HALVES - 1, 0))

        def finish(term, half):
            for chunk in range(CHUNKS):
                place = slice(chunk * part, (chunk + 1) * part)
                far_ready(term, half, chunk)
                value = r.normed_grad[half, :, place]
                for step in range(1, chips):
                    value = value + r.far_in[term, half, step - 1, :, place].astype(full)
                r.normed_grad[half, :, place] = value
            scaled = r.scaled[half]
            weighted = r.gain[...] * r.normed_grad[half]
            inner = jnp.sum(weighted * scaled, axis=1, keepdims=True)
            cotangent = inv_rms[half] * (weighted - scaled * (inner / width))
            if term == 0:
                adjoint_out[half] = cotangent
            else:
                adjoint_out[half] += cotangent
            if term < ITERS - 1:
                r.series[term, half, me] = cotangent.astype(low)
                gather_start((term + 1, half))

        for term in range(ITERS):
            if term:
                r.total[:, :, :, :head_width] = jnp.zeros(spread_rows, full)
                for half in range(HALVES):
                    gather_each((term, half), pull(term, half))
                    late_start(term, half)
                for half in range(HALVES):
                    late_whole(term, half).wait_recv()
            else:
                heads_ready(2)
                heads_ready(3)
            backward(term)
            push(term)
            for half in range(HALVES):
                finish(term, half)

        for item in range(3):
            gather_drain(item)
        for item in range(4):
            heads_drain(item)
        for item in range(2 * ITERS):
            grads_drain(item)
        for term in range(ITERS):
            for half in range(HALVES):
                query_whole(term, half).wait_send()
                if term:
                    gather_drain((term, half))
                    late_whole(term, half).wait_send()
        for term in range(ITERS):
            reduce_drain(term)
        block = r.gain_far.at[pl.ds(1, seq_count - 1)]
        remote(
            block, block, r.wide_send.at[0], r.wide_recv.at[0], "seq", flipped(me_seq, 1, bits)
        ).wait()
        value = r.gain_own[...]
        for mask in order:
            value = value + r.gain_far[mask]
        r.gain_mid[...] = value
        for step in range(1, tensor_count):
            near_copy(step).start()
        block = r.gain_near.at[pl.ds(1, tensor_count - 1)]
        remote(block, block, r.near_send.at[0], r.near_recv.at[0], "tensor", partner).wait()
        for step in range(1, tensor_count):
            value = value + r.gain_near[step]
        gain_out[...] = value

    anywhere = pl.BlockSpec(memory_space=pl.ANY)
    adjoint, gain_grad = pl.pallas_call(
        kernel,
        out_shape=[
            jax.ShapeDtypeStruct((HALVES, lines, width), full),
            jax.ShapeDtypeStruct((gain_rows, HEAD_DIM), full),
        ],
        in_specs=[anywhere] * 10,
        out_specs=[pl.BlockSpec(memory_space=pltpu.VMEM)] * 2,
        scratch_shapes=list(scratch.values()),
        compiler_params=pltpu.CompilerParams(
            collective_id=0, has_side_effects=True, vmem_limit_bytes=58 << 20
        ),
    )(
        fixed_point,
        incoming,
        norm_gain.reshape(1, width),
        query_weight.reshape(CHUNKS, part, head_width),
        key_weight.reshape(CHUNKS, part, head_width),
        value_weight.reshape(CHUNKS, part, head_width),
        out_weight,
        layout,
        jnp.asarray(cosine),
        jnp.asarray(sine),
    )

    def close(incoming_hbm, part_hbm, gain_hbm, adjoint_ref, scaled_ref, base, other, gain, sems):
        copies = [
            pltpu.make_async_copy(incoming_hbm, base, sems.at[0]),
            pltpu.make_async_copy(part_hbm, other, sems.at[1]),
            pltpu.make_async_copy(gain_hbm, gain, sems.at[2]),
        ]
        for copy in copies:
            copy.start()
        for copy in copies:
            copy.wait()
        adjoint_ref[...] = base[...].astype(full) + other[...].reshape(rows, width)
        scaled_ref[...] = gain[...] * length ** (-0.5)

    adjoint, gain_grad = pl.pallas_call(
        close,
        out_shape=[
            jax.ShapeDtypeStruct((rows, width), full),
            jax.ShapeDtypeStruct((gain_rows, HEAD_DIM), full),
        ],
        in_specs=[anywhere] * 3,
        out_specs=[pl.BlockSpec(memory_space=pltpu.VMEM)] * 2,
        scratch_shapes=[
            pltpu.VMEM((rows, width), low),
            pltpu.VMEM((HALVES, lines, width), full),
            pltpu.VMEM((gain_rows, HEAD_DIM), full),
            dma((3,)),
        ],
        compiler_params=pltpu.CompilerParams(vmem_limit_bytes=60 << 20),
    )(incoming, adjoint, gain_grad)
    return adjoint, gain_grad.reshape(width)


def solution(mesh):
    in_specs = (
        P(("seq", "tensor"), None),
        P(("seq", "tensor"), None),
        P(),
        P(None, "tensor"),
        P(None, "tensor"),
        P(None, "tensor"),
        P("tensor", None),
        P(),
    )
    out_specs = (P(("seq", "tensor"), None), P())
    seq, tensor = mesh.shape["seq"], mesh.shape["tensor"]

    def body(*arrays):
        heads = arrays[3].shape[1] * tensor // HEAD_DIM
        tokens = arrays[0].shape[0] * tensor
        fits = (
            tensor % 2 == 0
            and tensor >= 4
            and seq & (seq - 1) == 0
            and heads == seq * tensor
            and tokens % 128 == 0
            and arrays[0].shape[0] % (16 * HALVES) == 0
            and arrays[0].shape[1] == CHUNKS * arrays[3].shape[1]
            and arrays[3].shape[1] % (8 * HEAD_DIM) == 0
        )
        return (fused_body if fits else ring_body)(*arrays)

    return jax.shard_map(body, mesh=mesh, in_specs=in_specs, out_specs=out_specs, check_vma=False)
```

```python
import types

import jax
import jax.numpy as jnp
import numpy as np
from jax import lax
from jax.experimental import pallas as pl
from jax.experimental.pallas import tpu as pltpu
from jax.sharding import PartitionSpec as P

HEAD_DIM = 128
BLK = 64
ITERS = 2


EPS = 1e-05
THETA = 10000.0
MASKED = -1e30


def rope_tables(positions):
    freq = THETA ** (-jnp.arange(0, HEAD_DIM, 2, dtype=jnp.float32) / HEAD_DIM)
    angle = positions.astype(jnp.float32)[:, None] * freq[None, :]
    cosine = jnp.concatenate([jnp.cos(angle), jnp.cos(angle)], axis=1)[:, None, :]
    sine = jnp.concatenate([jnp.sin(angle), jnp.sin(angle)], axis=1)[:, None, :]
    return (cosine, sine)


def rotate(values, cosine, sine):
    half = HEAD_DIM // 2
    turned = jnp.concatenate([-values[..., half:], values[..., :half]], axis=-1)
    return values * cosine + turned * sine


def rotate_back(values, cosine, sine):
    half = HEAD_DIM // 2
    weighted = values * sine
    turned = jnp.concatenate([weighted[..., half:], -weighted[..., :half]], axis=-1)
    return values * cosine + turned


def expand_blocks(chosen):
    return jnp.repeat(jnp.repeat(chosen, BLK, axis=0), BLK, axis=1)


def pair_mask(query_pos, key_pos, chosen):
    query_block = (query_pos // BLK)[:, None]
    key_block = (key_pos // BLK)[None, :]
    earlier = (key_block < query_block) & chosen
    same = (key_block == query_block) & (key_pos[None, :] <= query_pos[:, None])
    return earlier | same


def ring_body(
    fixed_point, incoming, norm_gain, query_weight, key_weight, value_weight, out_weight, layout
):
    local_rows, model_width = fixed_point.shape
    head_width = query_weight.shape[1]
    head_count = head_width // HEAD_DIM
    seq_tokens = local_rows * lax.axis_size("tensor")
    seq_length = seq_tokens * lax.axis_size("seq")
    seq_index = lax.axis_index("seq")
    score_scale = HEAD_DIM ** (-0.5)
    contract_last = (((1,), (1,)), ((), ()))
    head_shape = (seq_tokens, head_count, HEAD_DIM)
    point = fixed_point.astype(jnp.float32)
    inv_rms = lax.rsqrt(jnp.mean(point * point, axis=1, keepdims=True) + EPS)
    scaled = point * inv_rms
    normed = (norm_gain * scaled).astype(jnp.bfloat16)
    project_piece = lax.all_gather(normed, "tensor", axis=0, tiled=True)
    projected = jnp.concatenate(
        [
            jnp.dot(project_piece, query_weight, preferred_element_type=jnp.float32),
            jnp.dot(project_piece, key_weight, preferred_element_type=jnp.float32),
            jnp.dot(project_piece, value_weight, preferred_element_type=jnp.float32),
        ],
        axis=1,
    )
    positions = seq_index * seq_tokens + jnp.arange(seq_tokens, dtype=jnp.int32)
    cosine, sine = rope_tables(positions)
    queries = rotate(projected[:, :head_width].reshape(head_shape), cosine, sine).astype(
        jnp.bfloat16
    )
    keys = rotate(
        projected[:, head_width : 2 * head_width].reshape(head_shape), cosine, sine
    ).astype(jnp.bfloat16)
    values = projected[:, 2 * head_width :].reshape(head_shape).astype(jnp.bfloat16)
    block_rows = seq_tokens // BLK
    block_count = seq_length // BLK
    first_block = seq_index * block_rows
    key_positions = jnp.arange(seq_length, dtype=jnp.int32)
    chosen_rows = (
        lax.dynamic_slice(layout, (first_block, jnp.int32(0)), (block_rows, block_count)) > 0
    )
    allowed = pair_mask(positions, key_positions, expand_blocks(chosen_rows))
    keys_all, values_all = (
        lax.all_gather(keys, "seq", axis=0, tiled=True),
        lax.all_gather(values, "seq", axis=0, tiled=True),
    )
    scores = (
        jnp.einsum("qhd,khd->hqk", queries, keys_all, preferred_element_type=jnp.float32)
        * score_scale
    )
    scores = jnp.where(allowed[None], scores, MASKED)
    log_norm = jax.nn.logsumexp(scores, axis=2, keepdims=True)
    probs = jnp.exp(scores - log_norm)
    probs_low = probs.astype(jnp.bfloat16)
    attended = jnp.einsum(
        "hqk,khd->qhd", probs_low, values_all, preferred_element_type=jnp.float32
    ).astype(jnp.bfloat16)
    cotangent = incoming.astype(jnp.float32)
    adjoint = cotangent
    gain_grad = jnp.zeros((model_width,), jnp.float32)
    for term_index in range(ITERS):
        grad_out = lax.dot_general(
            lax.all_gather(cotangent.astype(jnp.bfloat16), "tensor", axis=0, tiled=True),
            out_weight,
            contract_last,
            preferred_element_type=jnp.float32,
        )
        grad_low = grad_out.astype(jnp.bfloat16).reshape(head_shape)
        delta = jnp.sum(grad_low.astype(jnp.float32) * attended.astype(jnp.float32), axis=2)
        grad_probs = jnp.einsum(
            "qhd,khd->hqk", grad_low, values_all, preferred_element_type=jnp.float32
        )
        grad_scores = (probs * (grad_probs - delta.T[:, :, None])).astype(jnp.bfloat16)
        grad_query = (
            jnp.einsum("hqk,khd->qhd", grad_scores, keys_all, preferred_element_type=jnp.float32)
            * score_scale
        )
        key_part = (
            jnp.einsum("hqk,qhd->khd", grad_scores, queries, preferred_element_type=jnp.float32)
            * score_scale
        )
        value_part = jnp.einsum(
            "hqk,qhd->khd", probs_low, grad_low, preferred_element_type=jnp.float32
        )
        key_grads = lax.psum_scatter(
            jnp.concatenate(
                [
                    key_part.reshape(seq_tokens * lax.axis_size("seq"), head_width),
                    value_part.reshape(seq_tokens * lax.axis_size("seq"), head_width),
                ],
                axis=1,
            ).astype(jnp.bfloat16),
            "seq",
            scatter_dimension=0,
            tiled=True,
        ).astype(jnp.float32)
        grad_key = key_grads[:, :head_width].reshape(head_shape)
        grad_value = key_grads[:, head_width:].reshape(head_shape)
        query_low = (
            rotate_back(grad_query, cosine, sine)
            .astype(jnp.bfloat16)
            .reshape(seq_tokens, head_width)
        )
        key_low = (
            rotate_back(grad_key, cosine, sine).astype(jnp.bfloat16).reshape(seq_tokens, head_width)
        )
        value_low = grad_value.astype(jnp.bfloat16).reshape(seq_tokens, head_width)
        total = lax.dot_general(
            query_low, query_weight, contract_last, preferred_element_type=jnp.float32
        )
        total = total + lax.dot_general(
            key_low, key_weight, contract_last, preferred_element_type=jnp.float32
        )
        total = total + lax.dot_general(
            value_low, value_weight, contract_last, preferred_element_type=jnp.float32
        )
        grad_normed = lax.psum_scatter(
            total.astype(jnp.bfloat16), "tensor", scatter_dimension=0, tiled=True
        ).astype(jnp.float32)
        gain_term = jnp.sum(grad_normed * scaled, axis=0)
        gain_grad = gain_grad + lax.psum(gain_term, ("seq", "tensor"))
        weighted = norm_gain * grad_normed
        inner = jnp.sum(weighted * scaled, axis=1, keepdims=True)
        cotangent = inv_rms * (weighted - scaled * (inner / model_width))
        adjoint = adjoint + cotangent
    return (adjoint, gain_grad * seq_length ** (-0.5))


CHUNKS = 4
HALVES = 2
LAG = 2
MESH = pl.DeviceIdType.MESH


def numpy_tables(length):
    freq = np.float32(THETA) ** (-np.arange(0, HEAD_DIM, 2, dtype=np.float32) / np.float32(HEAD_DIM))
    angle = np.arange(length, dtype=np.float32)[:, None] * freq.astype(np.float32)[None, :]
    cosine = np.cos(angle.astype(np.float64)).astype(np.float32)
    sine = np.sin(angle.astype(np.float64)).astype(np.float32)
    return np.concatenate([cosine, cosine], axis=1), np.concatenate([-sine, sine], axis=1)


def product(left, right, left_dim, right_dim):
    return lax.dot_general(
        left, right, (((left_dim,), (right_dim,)), ((), ())), preferred_element_type=jnp.float32
    )


def flipped(index, mask, bits):
    result = 0
    for bit in range(bits):
        here = lax.rem(lax.div(index, 1 << bit), 2)
        result = result + (1 << bit) * ((1 - here) if (mask >> bit) & 1 else here)
    return result


def window(index, size):
    return pl.ds(pl.multiple_of(index * size, size), size)


def fused_body(
    fixed_point, incoming, norm_gain, query_weight, key_weight, value_weight, out_weight, layout
):
    rows, width = fixed_point.shape
    tensor_count = lax.axis_size("tensor")
    seq_count = lax.axis_size("seq")
    chips = tensor_count // 2
    bits = seq_count.bit_length() - 1
    head_width = query_weight.shape[1]
    tokens = rows * tensor_count
    length = tokens * seq_count
    blocks = layout.shape[0]
    part = width // CHUNKS
    lines = rows // HALVES
    groups = length // rows
    half_tokens = tensor_count * lines
    score_scale = HEAD_DIM ** (-0.5)
    gain_rows = width // HEAD_DIM
    gain_part = gain_rows // CHUNKS
    cosine, sine = numpy_tables(length)
    order = list(range(seq_count - 1, 0, -1))
    low, full = jnp.bfloat16, jnp.float32
    dma = pltpu.SemaphoreType.DMA
    scratch = {
        "weights": pltpu.VMEM((4 * CHUNKS + 1, part, head_width), low),
        "inverse": pltpu.VMEM((tokens, HEAD_DIM), full),
        "gain": pltpu.VMEM((1, width), full),
        "layout": pltpu.VMEM(layout.shape, jnp.int32),
        "cosine": pltpu.VMEM((length, HEAD_DIM), full),
        "sine": pltpu.VMEM((length, HEAD_DIM), full),
        "bias": pltpu.VMEM((blocks, length), full),
        "scaled": pltpu.VMEM((HALVES, lines, width), full),
        "pieces": pltpu.VMEM((3, tokens, width), low),
        "series": pltpu.VMEM((ITERS - 1, HALVES, tensor_count, lines, width), low),
        "heads_out": pltpu.VMEM((4, seq_count, tensor_count, HALVES, lines, HEAD_DIM), low),
        "heads_in": pltpu.VMEM((4, groups, HALVES, lines, HEAD_DIM), low),
        "late_out": pltpu.VMEM(
            (ITERS - 1, HALVES, seq_count, tensor_count, lines, HEAD_DIM), low
        ),
        "late_in": pltpu.VMEM((ITERS - 1, groups, HALVES, lines, HEAD_DIM), low),
        "probs": pltpu.VMEM((length, length), low),
        "key_acc": pltpu.VMEM((length, HEAD_DIM), full),
        "probs_turned": pltpu.VMEM((length, length), low),
        "grads_out": pltpu.VMEM((2 * ITERS, length, HEAD_DIM), low),
        "grads_in": pltpu.VMEM((2 * ITERS, tokens, head_width), low),
        "query_out": pltpu.VMEM((ITERS, groups, HALVES, lines, HEAD_DIM), low),
        "query_in": pltpu.VMEM((ITERS, HALVES, tensor_count, lines, head_width), low),
        "total": pltpu.VMEM((tensor_count, HALVES, lines, width), full),
        "hand_out": pltpu.VMEM((ITERS, HALVES, chips, lines, width), low),
        "hand_in": pltpu.VMEM((ITERS, HALVES, chips, lines, width), low),
        "far_out": pltpu.VMEM((ITERS, HALVES, chips - 1, lines, width), low),
        "far_in": pltpu.VMEM((ITERS, HALVES, chips - 1, lines, width), low),
        "normed_grad": pltpu.VMEM((HALVES, lines, width), full),
        "gain_sum": pltpu.VMEM((1, width), full),
        "gain_own": pltpu.VMEM((gain_rows, HEAD_DIM), full),
        "gain_near": pltpu.VMEM((tensor_count, gain_rows, HEAD_DIM), full),
        "gain_mid": pltpu.VMEM((gain_rows, HEAD_DIM), full),
        "gain_far": pltpu.VMEM((seq_count, gain_rows, HEAD_DIM), full),
        "load_sem": dma((6,)),
        "weight_sem": dma((CHUNKS + 1,)),
        "gather_send": dma((2 + HALVES,)),
        "gather_far": dma((2 + HALVES, CHUNKS * (chips - 1))),
        "gather_near": dma((2 + HALVES, CHUNKS)),
        "series_send": dma(((ITERS - 1) * HALVES,)),
        "series_far": dma(((ITERS - 1) * HALVES, CHUNKS * (chips - 1))),
        "series_near": dma(((ITERS - 1) * HALVES, CHUNKS)),
        "heads_send": dma((4,)),
        "heads_recv": dma((4,)),
        "late_send": dma(((ITERS - 1) * HALVES,)),
        "late_recv": dma(((ITERS - 1) * HALVES,)),
        "grads_send": dma((2 * ITERS,)),
        "grads_recv": dma((2 * ITERS,)),
        "query_send": dma((ITERS * HALVES,)),
        "query_recv": dma((ITERS * HALVES,)),
        "hand_send": dma((ITERS,)),
        "hand_recv": dma((ITERS * HALVES, CHUNKS)),
        "far_send": dma((ITERS,)),
        "far_recv": dma((ITERS * HALVES, CHUNKS)),
        "near_send": dma((1,)),
        "near_recv": dma((1,)),
        "wide_send": dma((1,)),
        "wide_recv": dma((1,)),
    }

    def kernel(*refs):
        point_hbm, incoming_hbm, gain_hbm, wq_hbm, wk_hbm, wv_hbm, wo_hbm = refs[:7]
        layout_hbm, cosine_hbm, sine_hbm, adjoint_out, gain_out = refs[7:12]
        r = types.SimpleNamespace(**dict(zip(scratch, refs[12:])))
        me_seq = lax.axis_index("seq")
        me = lax.axis_index("tensor")
        core = lax.rem(me, 2)
        chip = lax.div(me, 2)
        partner = me + 1 - 2 * core
        own_rows = window(me, rows)
        own_tokens = window(me_seq, tokens)
        own_columns = window(me_seq, HEAD_DIM)

        barrier = pltpu.get_barrier_semaphore()
        for step in range(1, tensor_count):
            pl.semaphore_signal(
                barrier,
                inc=1,
                device_id={"tensor": lax.rem(me + step, tensor_count)},
                device_id_type=MESH,
            )
        for mask in order:
            pl.semaphore_signal(
                barrier,
                inc=1,
                device_id={"seq": flipped(me_seq, mask, bits)},
                device_id_type=MESH,
            )

        def load(index, source, target):
            return pltpu.make_async_copy(source, target, r.load_sem.at[index])

        loads = [
            load(0, point_hbm, r.pieces.at[2, own_rows, :]),
            load(1, gain_hbm, r.gain),
            load(2, incoming_hbm, r.pieces.at[1, own_rows, :]),
            load(3, layout_hbm, r.layout),
            load(4, cosine_hbm, r.cosine),
            load(5, sine_hbm, r.sine),
        ]
        for copy in loads:
            copy.start()

        def block_of(item, chunk):
            return item * CHUNKS + chunk

        def weight_load(item, chunk):
            if item == 3:
                source = wo_hbm.at[:, window(chunk, part)]
            else:
                source = (wv_hbm, wk_hbm, wq_hbm)[item].at[chunk]
            target = r.weights.at[1 + block_of(item, chunk)]
            return pltpu.make_async_copy(
                source, target, r.weight_sem.at[CHUNKS if item == 3 else chunk]
            )

        def weight_ready(index, count):
            pltpu.make_async_copy(
                wq_hbm.at[pl.ds(0, count)], r.weights.at[pl.ds(0, count)], r.weight_sem.at[index]
            ).wait()

        def turn_weights(first, last):
            def body(block, carry):
                for line in range(0, part, HEAD_DIM):
                    strip = slice(line, line + HEAD_DIM)
                    r.weights[block, :, strip] = r.weights[block + 1, strip, :].T
                return carry

            lax.fori_loop(first * CHUNKS, last * CHUNKS, body, 0)

        def remote(source, target, send, recv, axis, peer):
            return pltpu.make_async_remote_copy(
                src_ref=source,
                dst_ref=target,
                send_sem=send,
                recv_sem=recv,
                device_id={axis: peer},
                device_id_type=MESH,
            )

        def gather_parts(item, chunk, origin):
            place = window(chunk, part)
            if isinstance(item, tuple):
                term, half = item
                if term == 0:
                    index = 0 if half == 0 else 2 + half
                    start = pl.multiple_of(origin * rows + half * lines, lines)
                    block = r.pieces.at[0, pl.ds(start, lines), place]
                    return block, r.gather_send.at[index], r.gather_far, r.gather_near, index
                index = (term - 1) * HALVES + half
                block = r.series.at[term - 1, half, origin, :, place]
                return block, r.series_send.at[index], r.series_far, r.series_near, index
            block = r.pieces.at[item, window(origin, rows), place]
            return block, r.gather_send.at[item], r.gather_far, r.gather_near, item

        def gather_far(item, chunk, step):
            block, send, far, near, index = gather_parts(item, chunk, me)
            recv = far.at[index, chunk * (chips - 1) + step - 1]
            peer = 2 * lax.rem(chip + step, chips) + core
            return remote(block, block, send, recv, "tensor", peer)

        def gather_near(item, chunk):
            block, send, far, near, index = gather_parts(item, chunk, me)
            return remote(block, block, send, near.at[index, chunk], "tensor", partner)

        def gather_pass(item, chunk, step):
            origin = 2 * lax.rem(chip + chips - step, chips) + core
            block, send, far, near, index = gather_parts(item, chunk, origin)
            return remote(block, block, send, near.at[index, chunk], "tensor", partner)

        def gather_start(item):
            for chunk in range(CHUNKS):
                for step in range(1, chips):
                    gather_far(item, chunk, step).start()
                gather_near(item, chunk).start()

        def gather_relay(item, chunk):
            for step in range(1, chips):
                gather_far(item, chunk, step).wait_recv()
                gather_pass(item, chunk, step).start()

        def gather_ready(item, chunk):
            place = window(chunk, part)
            block, send, far, near, index = gather_parts(item, chunk, 0)
            if isinstance(item, tuple) and item[0] == 0:
                block = r.pieces.at[0, pl.ds(0, chips * lines), place]
            elif isinstance(item, tuple):
                block = r.series.at[item[0] - 1, item[1], pl.ds(0, chips), :, place]
            else:
                block = r.pieces.at[item, pl.ds(0, chips * rows), place]
            remote(block, block, send, near.at[index, chunk], "tensor", partner).wait_recv()

        def gather_drain(item):
            block, send, far, near, index = gather_parts(item, 0, 0)
            if isinstance(item, tuple) and item[0] == 0:
                block = r.pieces.at[0, pl.ds(0, (2 * chips - 1) * lines), :]
            elif isinstance(item, tuple):
                block = r.series.at[item[0] - 1, item[1], pl.ds(0, 2 * chips - 1)]
            else:
                block = r.pieces.at[item, pl.ds(0, (2 * chips - 1) * rows), :]
            remote(block, block, send, near.at[index, 0], "tensor", partner).wait_send()

        def gather_each(item, use, after=None, count=CHUNKS):
            gather_relay(item, 0)

            def body(chunk, carry):
                @pl.when(chunk + 1 < CHUNKS)
                def _():
                    gather_relay(item, chunk + 1)

                if after is not None:

                    @pl.when(chunk + 2 == CHUNKS)
                    def _():
                        after()

                gather_ready(item, chunk)
                use(chunk)
                return carry

            lax.fori_loop(0, count, body, 0)

        def columns_of(slot):
            return slice(slot * head_width, (slot + 1) * head_width)

        def heads_copy(item, mask, half=None):
            source = r.heads_out.at[item, mask]
            target = r.heads_in.at[item, window(me_seq, tensor_count)]
            if half is not None:
                source, target = source.at[:, half], target.at[:, half]
            return remote(
                source,
                target,
                r.heads_send.at[item],
                r.heads_recv.at[item],
                "seq",
                flipped(me_seq, mask, bits),
            )

        def heads_start(item, turn, half=None):
            part_rows = slice(None) if half is None else slice(half, half + 1)
            count = tokens if half is None else half_tokens

            def table(values):
                values = values.reshape(tensor_count, HALVES, lines, HEAD_DIM)
                return values[:, part_rows].reshape(count, HEAD_DIM)

            for mask in order + [0]:
                peer = flipped(me_seq, mask, bits)
                columns = window(item * seq_count + peer, HEAD_DIM)
                values = r.total[:, part_rows, :, columns].reshape(count, HEAD_DIM)
                if turn:
                    values = values * table(r.cosine[own_tokens, :]) + pltpu.roll(
                        values, HEAD_DIM // 2, 1
                    ) * table(r.sine[own_tokens, :])
                values = values.astype(low).reshape(tensor_count, -1, lines, HEAD_DIM)
                if mask:
                    r.heads_out[item, mask, :, part_rows] = values
                else:
                    r.heads_in[item, window(me_seq, tensor_count), part_rows] = values
            for mask in order:
                heads_copy(item, mask, half).start()

        def late_copy(term, half, mask):
            index = (term - 1) * HALVES + half
            return remote(
                r.late_out.at[term - 1, half, mask],
                r.late_in.at[term - 1, window(me_seq, tensor_count), half],
                r.late_send.at[index],
                r.late_recv.at[index],
                "seq",
                flipped(me_seq, mask, bits),
            )

        def late_start(term, half):
            for mask in order + [0]:
                columns = window(flipped(me_seq, mask, bits), HEAD_DIM)
                values = r.total[:, half, :, columns].astype(low)
                if mask:
                    r.late_out[term - 1, half, mask] = values
                else:
                    r.late_in[term - 1, window(me_seq, tensor_count), half] = values
            for mask in order:
                late_copy(term, half, mask).start()

        def late_whole(term, half):
            block = r.late_out.at[term - 1, half, pl.ds(1, seq_count - 1)]
            index = (term - 1) * HALVES + half
            send, recv = r.late_send.at[index], r.late_recv.at[index]
            return remote(block, block, send, recv, "seq", flipped(me_seq, 1, bits))

        def heads_ready(item):
            block = r.heads_in.at[item, pl.ds(0, (seq_count - 1) * tensor_count)]
            send, recv = r.heads_send.at[item], r.heads_recv.at[item]
            remote(block, block, send, recv, "seq", flipped(me_seq, 1, bits)).wait_recv()

        def heads_drain(item):
            block = r.heads_out.at[item, pl.ds(1, seq_count - 1)]
            send, recv = r.heads_send.at[item], r.heads_recv.at[item]
            remote(block, block, send, recv, "seq", flipped(me_seq, 1, bits)).wait_send()

        def grads_copy(item, mask):
            peer = flipped(me_seq, mask, bits)
            return remote(
                r.grads_out.at[item, window(peer, tokens), :],
                r.grads_in.at[item, :, own_columns],
                r.grads_send.at[item],
                r.grads_recv.at[item],
                "seq",
                peer,
            )

        def grads_start(item):
            for mask in order:
                grads_copy(item, mask).start()
            r.grads_in[item, :, own_columns] = r.grads_out[item, own_tokens, :]

        def grads_ready(item):
            block = r.grads_in.at[item, :, pl.ds(0, (seq_count - 1) * HEAD_DIM)]
            send, recv = r.grads_send.at[item], r.grads_recv.at[item]
            remote(block, block, send, recv, "seq", flipped(me_seq, 1, bits)).wait_recv()

        def grads_drain(item):
            block = r.grads_out.at[item, pl.ds(0, (seq_count - 1) * tokens), :]
            send, recv = r.grads_send.at[item], r.grads_recv.at[item]
            remote(block, block, send, recv, "seq", flipped(me_seq, 1, bits)).wait_send()

        def query_copy(term, half, mask):
            peer = flipped(me_seq, mask, bits)
            index = term * HALVES + half
            return remote(
                r.query_out.at[term, window(peer, tensor_count), half],
                r.query_in.at[term, half, :, :, own_columns],
                r.query_send.at[index],
                r.query_recv.at[index],
                "seq",
                peer,
            )

        def query_start(term):
            for half in range(HALVES):
                for mask in order:
                    query_copy(term, half, mask).start()
                own = r.query_out[term, window(me_seq, tensor_count), half]
                r.query_in[term, half, :, :, own_columns] = own

        def query_whole(term, half):
            block = r.query_in.at[term, half, :, :, pl.ds(0, (seq_count - 1) * HEAD_DIM)]
            index = term * HALVES + half
            send, recv = r.query_send.at[index], r.query_recv.at[index]
            return remote(block, block, send, recv, "seq", flipped(me_seq, 1, bits))

        def hand_copy(term, half, chunk):
            place = window(chunk, part)
            return remote(
                r.hand_out.at[term, half, :, :, place],
                r.hand_in.at[term, half, :, :, place],
                r.hand_send.at[term],
                r.hand_recv.at[term * HALVES + half, chunk],
                "tensor",
                partner,
            )

        def far_copy(term, half, step, chunk):
            place = window(chunk, part)
            return remote(
                r.far_out.at[term, half, step - 1, :, place],
                r.far_in.at[term, half, step - 1, :, place],
                r.far_send.at[term],
                r.far_recv.at[term * HALVES + half, chunk],
                "tensor",
                2 * lax.rem(chip + step, chips) + core,
            )

        def far_ready(term, half, chunk):
            block = r.far_in.at[term, half, :, :, window(chunk, part)]
            send, recv = r.far_send.at[term], r.far_recv.at[term * HALVES + half, chunk]
            remote(block, block, send, recv, "tensor", partner).wait_recv()

        def reduce_drain(term):
            block = r.hand_out.at[term]
            send, recv = r.hand_send.at[term], r.hand_recv.at[term * HALVES, 0]
            remote(block, block, send, recv, "tensor", partner).wait_send()
            block = r.far_out.at[term]
            send, recv = r.far_send.at[term], r.far_recv.at[term * HALVES, 0]
            remote(block, block, send, recv, "tensor", partner).wait_send()

        def wide_copy(mask, chunk):
            place = window(chunk, gain_part)
            return remote(
                r.gain_own.at[place, :],
                r.gain_far.at[mask, place, :],
                r.wide_send.at[0],
                r.wide_recv.at[0],
                "seq",
                flipped(me_seq, mask, bits),
            )

        def near_copy(step):
            return remote(
                r.gain_mid,
                r.gain_near.at[step],
                r.near_send.at[0],
                r.near_recv.at[0],
                "tensor",
                lax.rem(me + step, tensor_count),
            )

        for copy in loads[:3]:
            copy.wait()
        for chunk in range(CHUNKS):
            for item in range(3):
                weight_load(item, chunk).start()
        for chunk in range(CHUNKS):
            weight_load(3, chunk).start()

        point = r.pieces[2, own_rows, :].astype(full).reshape(HALVES, lines, width)
        inv_rms = lax.rsqrt(jnp.mean(point * point, axis=-1, keepdims=True) + EPS)
        r.scaled[...] = point * inv_rms
        normed = r.gain[...].reshape(1, 1, width) * r.scaled[...]
        r.pieces[0, own_rows, :] = normed.astype(low).reshape(rows, width)
        pl.semaphore_wait(barrier, tensor_count - 1 + seq_count - 1)
        for half in range(HALVES):
            gather_start((0, half))

        loads[3].wait()
        spread = (
            lax.broadcasted_iota(jnp.int32, (blocks, length), 1) // BLK
            == lax.broadcasted_iota(jnp.int32, (blocks, length), 0)
        )
        chosen = product(
            jnp.where(r.layout[...] > 0, 1.0, 0.0).astype(low),
            jnp.where(spread, 1.0, 0.0).astype(low),
            1,
            0,
        )
        earlier = (
            lax.broadcasted_iota(jnp.int32, (blocks, length), 1) // BLK
            < lax.broadcasted_iota(jnp.int32, (blocks, length), 0)
        )
        r.bias[...] = jnp.where(earlier & (chosen > 0.5), 0.0, MASKED)
        r.total[...] = jnp.zeros(r.total.shape, full)
        spread_rows = (tensor_count, HALVES, lines, head_width)

        def project_one(item, half, chunk):
            place = window(chunk, part)
            starts = [owner * rows + half * lines for owner in range(tensor_count)]
            piece = jnp.concatenate(
                [r.pieces[0, start : start + lines, place] for start in starts], axis=0
            )
            weight = r.weights[1 + block_of(2 - item, chunk)]
            value = product(piece, weight, 1, 0)
            value = value.reshape(tensor_count, lines, head_width)
            r.total[:, half, :, columns_of(item)] += value

        def project(item, half):
            def body(chunk, carry):
                project_one(item, half, chunk)
                return carry

            lax.fori_loop(0, CHUNKS, body, 0)
            heads_start(item, item < 2, half)

        def project_first(chunk):
            weight_ready(chunk, 3)
            project_one(0, 0, chunk)

        gather_each((0, 0), project_first)
        for copy in loads[4:]:
            copy.wait()
        heads_start(0, True, 0)
        project(1, 0)
        for half in range(1, HALVES):
            for chunk in range(CHUNKS):
                gather_relay((0, half), chunk)
        gather_start(1)
        project(2, 0)
        for half in range(1, HALVES):
            for chunk in range(CHUNKS):
                gather_ready((0, half), chunk)
            for item in range(3):
                project(item, half)
        weight_ready(CHUNKS, CHUNKS)

        def pull_first(chunk):
            place = window(chunk, part)
            weight = r.weights[1 + block_of(3, chunk)]
            value = product(r.pieces[1, :, place], weight, 1, 1)
            r.total[:, :, :, columns_of(3)] += value.reshape(spread_rows)

        gather_each(1, pull_first)
        heads_start(3, False)

        def pull(term, half):
            def use(chunk):
                place = window(chunk, part)
                piece = r.series[term - 1, half, :, :, place].reshape(half_tokens, part)
                value = product(piece, r.weights[block_of(3, chunk)], 1, 0)
                r.total[:, half, :, :head_width] += value.reshape(tensor_count, lines, head_width)

            return use
        gather_start(2)
        turn_weights(0, 1)

        group = 2 if seq_count % 2 == 0 else 1
        heads_ready(0)
        heads_ready(1)
        sub = tokens // BLK

        def head_rows(item, first, count):
            block = r.heads_in[item, pl.ds(first * tensor_count, count * tensor_count)]
            return block.reshape(count * tokens, HEAD_DIM)

        def forward(base):
            span = (base + group) * tokens

            def body(step, carry):
                place = window(base + step, tokens)
                scores = product(
                    head_rows(0, base + step, 1), head_rows(1, 0, base + group), 1, 1
                ) * score_scale
                query_at = (base + step) * tokens + lax.broadcasted_iota(jnp.int32, (tokens, span), 0)
                key_at = lax.broadcasted_iota(jnp.int32, (tokens, span), 1)
                same = (query_at // BLK == key_at // BLK) & (key_at <= query_at)
                bias = jnp.concatenate(
                    [
                        jnp.broadcast_to(r.bias[pl.ds((base + step) * sub + line, 1), :span], (BLK, span))
                        for line in range(sub)
                    ],
                    axis=0,
                )
                scores = scores + jnp.where(same, 0.0, bias)
                top = jnp.max(scores, axis=1, keepdims=True)
                weight = jnp.exp(scores - top)
                weight = weight / jnp.sum(weight, axis=1, keepdims=True)
                r.probs[place, :span] = weight.astype(low)
                r.probs_turned[:span, place] = weight.T.astype(low)
                return carry

            lax.fori_loop(0, group, body, 0)

        for base in range(0, seq_count, group):
            forward(base)

        def turned_back(values, place):
            return (
                values * r.cosine[place, :]
                - pltpu.roll(values, HEAD_DIM // 2, 1) * r.sine[place, :]
            ).astype(low)

        def grad_rows(term, first, count):
            if term == 0:
                return head_rows(3, first, count)
            block = r.late_in[term - 1, pl.ds(first * tensor_count, count * tensor_count)]
            return block.reshape(count * tokens, HEAD_DIM)

        def backward(term):
            r.key_acc[...] = jnp.zeros(r.key_acc.shape, full)
            for base in range(0, seq_count, group):
                later = slice(base * tokens, length)
                for step in range(group):
                    place = slice((base + step) * tokens, (base + step + 1) * tokens)
                    r.grads_out[2 * term + 1, place, :] = product(
                        r.probs_turned[place, later],
                        grad_rows(term, base, seq_count - base),
                        1,
                        0,
                    ).astype(low)
            grads_start(2 * term + 1)

            def at(base):
                span = (base + group) * tokens

                def body(step, carry):
                    at_block = base + group - 1 - step
                    place = window(at_block, tokens)
                    probs = r.probs[place, :span]
                    grad_low = grad_rows(term, at_block, 1)
                    grad_probs = product(grad_low, head_rows(2, 0, base + group), 1, 1)
                    wide = probs.astype(full)
                    delta = jnp.sum(wide * grad_probs, axis=1, keepdims=True)
                    grad_scores = (wide * (grad_probs - delta)).astype(low)
                    grad_query = product(grad_scores, head_rows(1, 0, base + group), 1, 0) * score_scale
                    r.query_out[term, window(at_block, tensor_count)] = turned_back(
                        grad_query, place
                    ).reshape(tensor_count, HALVES, lines, HEAD_DIM)
                    r.key_acc[:span, :] += product(grad_scores, head_rows(0, at_block, 1), 0, 0)
                    return carry

                lax.fori_loop(0, group, body, 0)

            for base in reversed(range(0, seq_count, group)):
                at(base)
            r.grads_out[2 * term] = turned_back(r.key_acc[...] * score_scale, slice(None))
            grads_start(2 * term)
            query_start(term)

        def hand_work(term, half, chunk):
            place = window(chunk, part)
            for step in range(chips):
                owner = 2 * lax.rem(chip + step, chips) + core
                handed = r.hand_in[term, half, step, :, place].astype(full)
                pair = r.total[owner, half, :, place] + handed
                if step:
                    r.far_out[term, half, step - 1, :, place] = pair.astype(low)
                else:
                    r.normed_grad[half, :, place] = pair

        def far_start(term, half, chunk):
            for step in range(1, chips):
                far_copy(term, half, step, chunk).start()

        def gain_on(term, half, chunk):
            place = window(chunk, part)
            gain_term = jnp.zeros((lines, part), full)
            for owner in range(tensor_count):
                own = slice(owner * rows + half * lines, owner * rows + (half + 1) * lines)
                scaled = r.pieces[2, own, place].astype(full) * r.inverse[own, :1]
                gain_term += r.total[owner, half, :, place] * scaled
            gain_term = jnp.sum(gain_term, axis=0, keepdims=True)
            if term + half:
                gain_term += r.gain_sum[:, place]
            if term < ITERS - 1 or half < HALVES - 1:
                r.gain_sum[:, place] = gain_term
                return
            r.gain_own[window(chunk, gain_part), :] = jnp.concatenate(
                [gain_term[:, line * HEAD_DIM : (line + 1) * HEAD_DIM] for line in range(gain_part)],
                axis=0,
            )
        def invert():
            for chunk in range(CHUNKS):
                gather_relay(2, chunk)
            for chunk in range(CHUNKS):
                gather_ready(2, chunk)
            for owner in range(tensor_count):
                place = slice(owner * rows, (owner + 1) * rows)
                point = r.pieces[2, place, :].astype(full)
                inverse = lax.rsqrt(jnp.mean(point * point, axis=1, keepdims=True) + EPS)
                r.inverse[place, :] = jnp.broadcast_to(inverse, (rows, HEAD_DIM))

        def push(term):
            if term == 0:
                turn_weights(1, 2)
            for item in (1, 0):
                if term == 0 and item == 0:
                    turn_weights(2, 3)
                    invert()
                grads_ready(2 * term + item)

                def body(chunk, carry):
                    place = window(chunk, part)
                    weight = r.weights[block_of(1 - item, chunk)]
                    value = product(r.grads_in[2 * term + item], weight, 1, 0)
                    value = value.reshape(tensor_count, HALVES, lines, part)
                    if item == 0:
                        value = value + r.total[:, :, :, place]
                    r.total[:, :, :, place] = value
                    return carry

                lax.fori_loop(0, CHUNKS, body, 0)

            def matmul(half, chunk):
                place = window(chunk, part)
                grads = r.query_in[term, half].reshape(half_tokens, head_width)
                value = product(grads, r.weights[block_of(2, chunk)], 1, 0)
                r.total[:, half, :, place] += value.reshape(tensor_count, lines, part)
                for step in range(chips):
                    other = 2 * lax.rem(chip + step, chips) + 1 - core
                    r.hand_out[term, half, step, :, place] = r.total[
                        other, half, :, place
                    ].astype(low)
                gain_on(term, half, chunk)

            def stage(half, first, last, behind):
                def body(chunk, carry):
                    if behind is not None:
                        earlier_half, shift = behind
                        hand_copy(term, earlier_half, chunk + shift).wait_recv()
                        hand_work(term, earlier_half, chunk + shift)
                        if term < ITERS - 1:
                            far_start(term, earlier_half, chunk + shift)
                    if half is not None:
                        matmul(half, chunk)
                        hand_copy(term, half, chunk).start()
                        if term == ITERS - 1 and half == HALVES - 1:
                            for mask in order:
                                wide_copy(mask, chunk).start()
                    if behind is not None and term == ITERS - 1:
                        far_start(term, earlier_half, chunk + shift)
                    return carry

                lax.fori_loop(first, last, body, 0)

            for half in range(HALVES):
                query_whole(term, half).wait_recv()
                stage(half, 0, LAG, (half - 1, CHUNKS - LAG) if half else None)
                stage(half, LAG, CHUNKS, (half, -LAG))
            stage(None, CHUNKS - LAG, CHUNKS, (HALVES - 1, 0))

        def finish(term, half):
            for chunk in range(CHUNKS):
                place = slice(chunk * part, (chunk + 1) * part)
                far_ready(term, half, chunk)
                value = r.normed_grad[half, :, place]
                for step in range(1, chips):
                    value = value + r.far_in[term, half, step - 1, :, place].astype(full)
                r.normed_grad[half, :, place] = value
            scaled = r.scaled[half]
            weighted = r.gain[...] * r.normed_grad[half]
            inner = jnp.sum(weighted * scaled, axis=1, keepdims=True)
            cotangent = inv_rms[half] * (weighted - scaled * (inner / width))
            if term == 0:
                adjoint_out[half] = cotangent
            else:
                adjoint_out[half] += cotangent
            if term < ITERS - 1:
                r.series[term, half, me] = cotangent.astype(low)
                gather_start((term + 1, half))

        for term in range(ITERS):
            if term:
                r.total[:, :, :, :head_width] = jnp.zeros(spread_rows, full)
                for half in range(HALVES):
                    gather_each((term, half), pull(term, half))
                    late_start(term, half)
                for half in range(HALVES):
                    late_whole(term, half).wait_recv()
            else:
                heads_ready(2)
                heads_ready(3)
            backward(term)
            push(term)
            for half in range(HALVES):
                finish(term, half)
                if term + half == 0:
                    turn_weights(3, 4)

        for item in [(0, half) for half in range(HALVES)] + [1, 2]:
            gather_drain(item)
        for item in range(4):
            heads_drain(item)
        for item in range(2 * ITERS):
            grads_drain(item)
        for term in range(ITERS):
            for half in range(HALVES):
                query_whole(term, half).wait_send()
                if term:
                    gather_drain((term, half))
                    late_whole(term, half).wait_send()
        for term in range(ITERS):
            reduce_drain(term)
        block = r.gain_far.at[pl.ds(1, seq_count - 1)]
        remote(
            block, block, r.wide_send.at[0], r.wide_recv.at[0], "seq", flipped(me_seq, 1, bits)
        ).wait()
        value = r.gain_own[...]
        for mask in order:
            value = value + r.gain_far[mask]
        r.gain_mid[...] = value
        for step in range(1, tensor_count):
            near_copy(step).start()
        block = r.gain_near.at[pl.ds(1, tensor_count - 1)]
        remote(block, block, r.near_send.at[0], r.near_recv.at[0], "tensor", partner).wait()
        for step in range(1, tensor_count):
            value = value + r.gain_near[step]
        gain_out[...] = value

    anywhere = pl.BlockSpec(memory_space=pl.ANY)
    adjoint, gain_grad = pl.pallas_call(
        kernel,
        out_shape=[
            jax.ShapeDtypeStruct((HALVES, lines, width), full),
            jax.ShapeDtypeStruct((gain_rows, HEAD_DIM), full),
        ],
        in_specs=[anywhere] * 10,
        out_specs=[pl.BlockSpec(memory_space=pltpu.VMEM)] * 2,
        scratch_shapes=list(scratch.values()),
        compiler_params=pltpu.CompilerParams(
            collective_id=0, has_side_effects=True, vmem_limit_bytes=58 << 20
        ),
    )(
        fixed_point,
        incoming,
        norm_gain.reshape(1, width),
        query_weight.reshape(CHUNKS, part, head_width),
        key_weight.reshape(CHUNKS, part, head_width),
        value_weight.reshape(CHUNKS, part, head_width),
        out_weight,
        layout,
        jnp.asarray(cosine),
        jnp.asarray(sine),
    )

    def close(incoming_hbm, part_hbm, gain_hbm, adjoint_ref, scaled_ref, base, other, gain, sems):
        copies = [
            pltpu.make_async_copy(incoming_hbm, base, sems.at[0]),
            pltpu.make_async_copy(part_hbm, other, sems.at[1]),
            pltpu.make_async_copy(gain_hbm, gain, sems.at[2]),
        ]
        for copy in copies:
            copy.start()
        for copy in copies:
            copy.wait()
        adjoint_ref[...] = base[...].astype(full) + other[...].reshape(rows, width)
        scaled_ref[...] = gain[...] * length ** (-0.5)

    adjoint, gain_grad = pl.pallas_call(
        close,
        out_shape=[
            jax.ShapeDtypeStruct((rows, width), full),
            jax.ShapeDtypeStruct((gain_rows, HEAD_DIM), full),
        ],
        in_specs=[anywhere] * 3,
        out_specs=[pl.BlockSpec(memory_space=pltpu.VMEM)] * 2,
        scratch_shapes=[
            pltpu.VMEM((rows, width), low),
            pltpu.VMEM((HALVES, lines, width), full),
            pltpu.VMEM((gain_rows, HEAD_DIM), full),
            dma((3,)),
        ],
        compiler_params=pltpu.CompilerParams(vmem_limit_bytes=60 << 20),
    )(incoming, adjoint, gain_grad)
    return adjoint, gain_grad.reshape(width)


def solution(mesh):
    in_specs = (
        P(("seq", "tensor"), None),
        P(("seq", "tensor"), None),
        P(),
        P(None, "tensor"),
        P(None, "tensor"),
        P(None, "tensor"),
        P("tensor", None),
        P(),
    )
    out_specs = (P(("seq", "tensor"), None), P())
    seq, tensor = mesh.shape["seq"], mesh.shape["tensor"]

    def body(*arrays):
        heads = arrays[3].shape[1] * tensor // HEAD_DIM
        tokens = arrays[0].shape[0] * tensor
        fits = (
            tensor % 2 == 0
            and tensor >= 4
            and seq & (seq - 1) == 0
            and heads == seq * tensor
            and tokens % 128 == 0
            and arrays[0].shape[0] % (16 * HALVES) == 0
            and arrays[0].shape[1] == CHUNKS * arrays[3].shape[1]
            and arrays[3].shape[1] % (8 * HEAD_DIM) == 0
        )
        return (fused_body if fits else ring_body)(*arrays)

    return jax.shard_map(body, mesh=mesh, in_specs=in_specs, out_specs=out_specs, check_vma=False)
```
